32 devices in a mesh: grp: 2 (over y), blk: 8 (over z, x), uly: 2 (over core).
Axes of the slice: x: 2, y: 2, z: 4, core: 2. Of those that a mesh axis runs over, the one named last changes fastest.
Arguments:
- query: bfloat16 [512, 1152], P(('grp', 'blk', 'uly')), parts along dimension 0, may hold values from -6 to 6
- key: bfloat16 [512, 1152], P(('grp', 'blk', 'uly')), parts along dimension 0, may hold values from -6 to 6
- value: bfloat16 [512, 1152], P(('grp', 'blk', 'uly')), parts along dimension 0, may hold values from -6 to 6
- q_gain: float32 [96], replicated, may hold values from 1 to 2.5
- k_gain: float32 [96], replicated, may hold values from 1 to 2.5
- out_weight: bfloat16 [1152, 2304], P('uly'), may hold values from -0.1875 to 0.1875
Outputs:
- mixed: bfloat16 [512, 2304], P(('grp', 'blk', 'uly')), parts along dimension 0
The draws below stay inside these ranges and needn't reach their ends.
There are 2 independent parts, one for each index of `grp`. The reference program is written for one: setup_inputs(seed, part) draws one part's arguments, and reference() takes and returns one part's arrays. A program takes and returns all parts, laid end to end along the dimension named above; an argument that names none is the same for every part. Nothing has to cross between parts.
All inputs are finite; a program needn't handle non-finite values.
Results may differ from the reference program's by a relative error of at most 0.012.
Values may be sent and summed in bfloat16 or wider, within the bound.
A program may use at most 128 MiB of HBM per device.

```python
import jax
import jax.numpy as jnp
from jax import lax

H = 12
HD = 96
D = 2304
S = 256


def steps_of(stream_key, extent, pieces, least, top_value):
    def one(position, shards_of):
        heights = jax.random.uniform(jax.random.fold_in(jax.random.fold_in(stream_key, 6), position), (shards_of,), jnp.float32, least / len(pieces), top_value / len(pieces))
        return jnp.repeat(jnp.exp(heights), extent[position] // shards_of).reshape((-1,) + (1,) * (len(extent) - position - 1))

    level = one(*pieces[0])
    for cut in pieces[1:]:
        level = level * one(*cut)
    return level


def normal_values(rng, shape, spread, most, shards=(), dtype=jnp.bfloat16):
    loudness = steps_of(rng, shape, shards, -0.22, 0.18) if shards else 1.0
    drawn = jax.random.normal(rng, shape, jnp.float32) * spread * loudness
    return jnp.minimum(jnp.maximum(drawn, -most), most).astype(dtype)


def setup_inputs(seed: int = 0, part: int = 0) -> dict:
    seeds = jax.random.split(jax.random.key(seed), 7)
    part_splits = jax.random.split(jax.random.fold_in(seeds[6], part), 7)
    query = normal_values(part_splits[0], (S, H * HD), 1.0, 6.0, ((0, 16),))
    key = normal_values(part_splits[1], (S, H * HD), 1.0, 6.0, ((0, 16),))
    value = normal_values(part_splits[2], (S, H * HD), 1.0, 6.0, ((0, 16),))
    q_gain = jnp.clip(jax.random.uniform(seeds[3], (HD,), jnp.float32, 1.0, 2.5), 1.0, 2.5)
    k_gain = jnp.clip(jax.random.uniform(seeds[4], (HD,), jnp.float32, 1.0, 2.5), 1.0, 2.5)
    out_weight = normal_values(seeds[5], (H * HD, D), (H * HD) ** -0.5, 0.1875, ((0, 2),))
    return {"query": query, "key": key, "value": value, "q_gain": q_gain, "k_gain": k_gain, "out_weight": out_weight}


def normed(data, gain):
    count = data.shape[0]
    grid = data.astype(jnp.float32).reshape(count, H, HD)
    meansq = lax.optimization_barrier(jnp.mean(grid * grid, axis=-1, keepdims=True))
    return (grid * lax.rsqrt(meansq + 1e-06) * gain).astype(jnp.bfloat16)

def reference(query, key, value, q_gain, k_gain, out_weight):
    count = query.shape[0]
    query_heads = jnp.transpose(normed(query, q_gain), (1, 0, 2))
    key_heads = jnp.transpose(normed(key, k_gain), (1, 0, 2))
    value_heads = jnp.transpose(value.reshape(count, H, HD), (1, 0, 2))
    score_scale = float(HD) ** (-0.5)

    def one_head(operands):
        query_one, key_one, value_one = operands
        scores = jnp.dot(query_one, key_one.T, preferred_element_type=jnp.float32) * score_scale
        expd = jnp.exp(scores)
        total_weight = lax.optimization_barrier(jnp.sum(expd, axis=1))
        weighted = jnp.dot(expd.astype(jnp.bfloat16), value_one, preferred_element_type=jnp.float32)
        return (weighted / total_weight[:, None]).astype(jnp.bfloat16)
    attn = lax.map(one_head, (query_heads, key_heads, value_heads))
    attn = jnp.transpose(attn, (1, 0, 2)).reshape(count, H * HD)
    return jnp.dot(attn, out_weight, preferred_element_type=jnp.float32).astype(jnp.bfloat16)
```

```python
import functools

import jax
import jax.numpy as jnp
from jax import lax
from jax.experimental import pallas as pl
from jax.experimental.pallas import tpu as pltpu
from jax.sharding import PartitionSpec as P

HD = 96
LANES = 128
CHUNKS = 1
GROUPS = 4
LOG2E = 1.4426950408889634
MESH = pl.DeviceIdType.MESH


def loop(count, body):
    if count <= 32:
        for i in range(count):
            body(i)
    else:
        lax.fori_loop(0, count, lambda i, c: (body(i), c)[1], 0)


def take(ref, sem):
    pltpu.make_async_copy(ref, ref, sem).wait()


def layer_kernel(
    blks, ulys, heads, copies,
    q_hbm, k_hbm, v_hbm, qg_hbm, kg_hbm, w_hbm, out_ref,
    raw, gains, w_vmem, pack, qkv, attn, back, acc,
    load_sem, gain_sem, w_sem, send1, recv1, send2, recv2, send_w, recv_w,
):
    n = blks * ulys
    rows = raw.shape[1]
    owners = heads * copies
    blk, uly = lax.axis_index("blk"), lax.axis_index("uly")
    me = blk * ulys + uly
    seq = n * rows
    block = seq // copies
    chunks = CHUNKS
    chunk = block // chunks
    groups = recv2.shape[0]
    members = heads // groups
    targets = chunk // rows
    depth = w_hbm.shape[0]
    upper = (2 * me) // n

    barrier = pltpu.get_barrier_semaphore()

    def greet(i):
        d = lax.rem(me + n // 2 + i + i // (n // 2), n)
        pl.semaphore_signal(
            barrier, inc=1, device_id={"blk": d // ulys, "uly": d % ulys}, device_id_type=MESH
        )

    loop(n - 1, greet)

    loads = [
        pltpu.make_async_copy(src, raw.at[i], load_sem.at[i])
        for i, src in enumerate((q_hbm, k_hbm, v_hbm))
    ]
    load_gains = [
        pltpu.make_async_copy(src, gains.at[i], gain_sem)
        for i, src in enumerate((qg_hbm, kg_hbm))
    ]
    for one in loads + load_gains:
        one.start()

    def mirror(d):
        plane = d // 4
        return d + (plane % 2) * (3 - 2 * (d % 4))

    def owner_device(o):
        return mirror(o * n // owners)

    spot = mirror(me)
    slot = (spot * owners + n - 1) // n
    is_owner = jnp.logical_and(slot < owners, (slot * n) // owners == spot)
    slot = jnp.minimum(slot, owners - 1)

    my_depth = pl.ds(pl.multiple_of(uly * depth, depth), depth)
    load_w = pltpu.make_async_copy(w_hbm, w_vmem.at[my_depth], w_sem)
    load_w.start()

    pad = jnp.zeros((rows, LANES - HD), jnp.bfloat16)
    take(gains, gain_sem)
    for i in range(2):
        loads[i].wait()
        gain = gains[i]
        for h in range(heads):
            x = raw[i, :, h * HD:(h + 1) * HD].astype(jnp.float32)
            scale = lax.rsqrt(jnp.mean(x * x, axis=-1, keepdims=True) + 1e-06)
            normed = (x * scale * gain).astype(jnp.bfloat16)
            pack[h, :, i * LANES:(i + 1) * LANES] = jnp.concatenate([normed, pad], axis=1)
    loads[2].wait()
    for h in range(heads):
        x = raw[2, :, h * HD:(h + 1) * HD]
        pack[h, :, 2 * LANES:3 * LANES] = jnp.concatenate([x, pad], axis=1)

    pl.semaphore_wait(barrier, n - 1)

    my_rows = pl.ds(pl.multiple_of(me * rows, rows), rows)

    def send_of(o):
        d = owner_device(o)
        return d, pltpu.make_async_remote_copy(
            src_ref=pack.at[o // copies],
            dst_ref=qkv.at[my_rows],
            send_sem=send1,
            recv_sem=recv1,
            device_id={"blk": d // ulys, "uly": d % ulys},
            device_id_type=MESH,
        )

    def send(i):
        d, copy = send_of(owners - 1 - i + upper * (2 * i + 1 - owners))

        @pl.when(d != me)
        def _():
            copy.start()

    loop(owners, send)

    give_w = pltpu.make_async_remote_copy(
        src_ref=w_hbm,
        dst_ref=w_vmem.at[my_depth],
        send_sem=send_w,
        recv_sem=recv_w,
        device_id={"blk": blk, "uly": 1 - uly},
        device_id_type=MESH,
    )
    give_w.start()

    @pl.when(is_owner)
    def _():
        head = slot // copies
        part = slot % copies
        qkv[my_rows, :] = pack[head]

        take(qkv.at[pl.ds(0, (n - 1) * rows)], recv1)
        score_scale = float(HD) ** (-0.5)

        def step(query, j, carry):
            weighted, total = carry
            here = pl.ds(j * block, block)
            keys = qkv[here, LANES:2 * LANES]
            values = qkv[here, 2 * LANES:3 * LANES]
            scores = lax.dot_general(
                query, keys, (((1,), (1,)), ((), ())), preferred_element_type=jnp.float32
            ) * score_scale
            expd = jnp.exp(scores)
            total = total + jnp.sum(expd, axis=-1, keepdims=True)
            weighted = weighted + jnp.dot(
                expd.astype(jnp.bfloat16), values, preferred_element_type=jnp.float32
            )
            return weighted, total

        def result_copies(c):
            for k in range(targets):
                i = targets - 1 - k + upper * (2 * k + 1 - targets)
                d = (part * chunks + c) * targets + i
                src = attn.at[pl.ds(pl.multiple_of((c * targets + i) * rows, rows), rows)]
                yield (
                    d == me,
                    functools.partial(
                        pltpu.make_async_copy, src, back.at[head], recv2.at[head // members]
                    ),
                    pltpu.make_async_remote_copy(
                        src_ref=src,
                        dst_ref=back.at[head],
                        send_sem=send2,
                        recv_sem=recv2.at[head // members],
                        device_id={"blk": d // ulys, "uly": d % ulys},
                        device_id_type=MESH,
                    ),
                )

        for k in range(chunks):
            c = chunks - 1 - k + upper * (2 * k + 1 - chunks)
            at = part * block + c * chunk
            query = qkv[pl.ds(pl.multiple_of(at, chunk), chunk), 0:LANES]
            carry = (jnp.zeros((chunk, LANES), jnp.float32), jnp.zeros((chunk, 1), jnp.float32))
            if copies == 1:
                weighted, total = step(query, 0, carry)
            else:
                weighted, total = lax.fori_loop(
                    0, copies, functools.partial(lambda q, j, c: step(q, j, c), query), carry
                )
            attn[pl.ds(pl.multiple_of(c * chunk, chunk), chunk), :] = (weighted / total).astype(jnp.bfloat16)
            for home, local, remote in result_copies(c):
                pl.when(home)(lambda local=local: local().start())
                pl.when(jnp.logical_not(home))(remote.start)

    load_w.wait()
    give_w.wait_recv()
    first = (me * groups) // n
    for i in range(groups):
        g = lax.rem(first + i * (1 - 2 * upper) + groups, groups)
        take(back.at[pl.ds(g * members, members)], recv2.at[g])
        for j in range(members):
            h = g * members + j
            term = jnp.dot(
                back[h, :, 0:HD],
                w_vmem[pl.ds(pl.multiple_of(h * HD, HD), HD), :],
                preferred_element_type=jnp.float32,
            )
            if i == 0 and j == 0:
                acc[...] = term
            elif i < groups - 1 or j < members - 1:
                acc[...] += term
            else:
                out_ref[...] = (acc[...] + term).astype(out_ref.dtype)

    give_w.wait_send()
    for i in range(copies - 1):
        take(pack, send1)

    @pl.when(is_owner)
    def _():
        take(pack.at[pl.ds(0, heads - 1)], send1)
        at_home = (slot % copies) * block == (me * rows) // block * block
        pl.when(at_home)(lambda: take(attn.at[pl.ds(0, block - rows)], send2))
        pl.when(jnp.logical_not(at_home))(lambda: take(attn, send2))

    @pl.when(jnp.logical_not(is_owner))
    def _():
        take(pack, send1)


def on_device(blks, ulys, query, key, value, q_gain, k_gain, out_weight):
    rows, width = query.shape
    heads = width // HD
    n = blks * ulys
    copies = 1
    while heads * copies * 2 <= n:
        copies *= 2
    owners = heads * copies
    depth, cols = out_weight.shape
    seq = n * rows
    block = seq // copies
    dma = pltpu.SemaphoreType.DMA
    return pl.pallas_call(
        functools.partial(layer_kernel, blks, ulys, heads, copies),
        out_shape=pltpu.VMEM((rows, cols), jnp.bfloat16),
        in_specs=[pl.BlockSpec(memory_space=pltpu.HBM)] * 6,
        out_specs=pl.BlockSpec(memory_space=pltpu.VMEM),
        scratch_shapes=[
            pltpu.VMEM((3, rows, width), jnp.bfloat16),
            pltpu.VMEM((2, 1, HD), jnp.float32),
            pltpu.VMEM((width, cols), jnp.bfloat16),
            pltpu.VMEM((heads, rows, 3 * LANES), jnp.bfloat16),
            pltpu.VMEM((seq, 3 * LANES), jnp.bfloat16),
            pltpu.VMEM((block, LANES), jnp.bfloat16),
            pltpu.VMEM((heads, rows, LANES), jnp.bfloat16),
            pltpu.VMEM((rows, cols), jnp.float32),
            dma((3,)),
            dma,
            dma,
            dma,
            dma,
            dma,
            dma((GROUPS,)),
            dma,
            dma,
        ],
        compiler_params=pltpu.CompilerParams(collective_id=0, has_side_effects=True),
    )(query, key, value, q_gain.reshape(1, HD), k_gain.reshape(1, HD), out_weight)


def pair_windows(width, heads):
    tiles = width // LANES
    span = (tiles + 1) // 2
    half = heads // 2
    sides = []
    for side in range(2):
        base = side * (tiles - span)
        one = []
        for j in range(half // 2):
            lane = (side * half + 2 * j) * HD
            tile = lane // LANES
            one.append((tile - base, lane - tile * LANES))
        sides.append(one)
    return span * LANES, (tiles - span) * LANES, sides


def gather_kernel(
    blks, heads,
    q_hbm, k_hbm, v_hbm, qg_hbm, kg_hbm, w_hbm, out_ref,
    raw, gains, normed, kbuf, vbuf, qbuf, attn, back, acc, w_vmem,
    load_sem, gain_sem, w_sem, send_v, send_k, send_q, send_a, send_w,
    recv_v, recv_k, recv_q, recv_a, recv_w, ready, sib,
):
    levels = blks // 2
    rows, width = raw.shape[1:]
    span, shift, sides = pair_windows(width, heads)
    group = 4 * rows
    half_levels = levels // 2
    part = half_levels * group
    blk, uly = lax.axis_index("blk"), lax.axis_index("uly")
    level, side = blk // 2, blk % 2
    me = blk * 2 + uly
    rank = level * 4 + side * 2 + 1 - uly
    half = level // half_levels
    owners = [(h, s, (half_levels - 1 + h) * 2 + s) for h in range(2) for s in range(2)]
    owner_ranks = [2 * b for _, _, b in owners]
    is_owner = functools.reduce(
        jnp.logical_or, [jnp.logical_and(uly == 1, blk == b) for _, _, b in owners]
    )
    my_rows = pl.ds(pl.multiple_of(me * rows, rows), rows)
    depth = w_hbm.shape[0]
    my_depth = pl.ds(pl.multiple_of(uly * depth, depth), depth)

    load_gains = [
        pltpu.make_async_copy(src, gains.at[i], gain_sem)
        for i, src in enumerate((qg_hbm, kg_hbm))
    ]
    loads = [
        pltpu.make_async_copy(src, raw.at[i], load_sem.at[i])
        for i, src in enumerate((q_hbm, k_hbm, v_hbm))
    ]
    for one in (loads[2], loads[1], *load_gains, loads[0]):
        one.start()

    barrier = pltpu.get_barrier_semaphore()
    everyone = [(l, s, c) for l in range(levels) for s in range(2) for c in (1, 0)]
    for l, s, c in everyone:
        other = l * 4 + s * 2 + 1 - c
        cond = other > rank
        if other not in owner_ranks:
            cond = jnp.logical_and(cond, jnp.logical_or(is_owner, blk == l * 2 + s))

        @pl.when(cond)
        def _(l=l, s=s, c=c):
            pl.semaphore_signal(
                barrier, inc=1, device_id={"blk": l * 2 + s, "uly": c}, device_id_type=MESH
            )

    load_w = pltpu.make_async_copy(w_hbm, w_vmem.at[my_depth], w_sem)
    load_w.start()

    heard = 1 - uly
    for r in owner_ranks:
        heard += jnp.logical_and(r < rank, r != rank - 1 + uly).astype(jnp.int32)
    heard = jnp.where(is_owner, rank, heard)
    pl.when(heard > 0)(lambda: pl.semaphore_wait(barrier, heard))

    for l, s, c in everyone:
        other = l * 4 + s * 2 + 1 - c

        @pl.when(jnp.logical_and(other < rank, is_owner))
        def _(l=l, s=s, c=c):
            pl.semaphore_signal(
                ready.at[blk], inc=1, device_id={"blk": l * 2 + s, "uly": c}, device_id_type=MESH
            )

    @pl.when(uly == 0)
    def _():
        pl.semaphore_signal(sib, inc=1, device_id={"uly": 1}, device_id_type=MESH)

    def lanes(s):
        return pl.ds(s * shift, span)

    def give(src, dst, owner, send, recv):
        _, s, b = owner
        return pltpu.make_async_remote_copy(
            src_ref=src.at[:, lanes(s)],
            dst_ref=dst,
            send_sem=send,
            recv_sem=recv,
            device_id={"blk": b, "uly": 1},
            device_id_type=MESH,
        )

    def give_v(owner):
        return give(raw.at[2], vbuf.at[my_rows], owner, send_v, recv_v.at[level])

    def give_k(owner):
        return give(normed.at[1], kbuf.at[my_rows], owner, send_k, recv_k.at[level])

    q_rows = pl.ds(pl.multiple_of((me - half * (2 * blks // 2)) * rows, rows), rows)

    def give_q(owner):
        return give(normed.at[0], qbuf.at[q_rows], owner, send_q, recv_q)

    def others(h, body):
        for owner in owners[2 * h + 1], owners[2 * h]:
            mine = jnp.logical_and(uly == 1, blk == owner[2])
            pl.when(jnp.logical_not(mine))(functools.partial(body, owner))

    def await_ready(h):
        for _, _, b in owners[2 * h:2 * h + 2]:
            pl.when(2 * b > rank)(lambda b=b: pl.semaphore_wait(ready.at[b], 1))

    def normalize(i):
        tiled = jnp.concatenate([gains[i]] * 4, axis=1)
        lane = lax.broadcasted_iota(jnp.int32, (rows, LANES), 1)
        for g in range(width // (3 * LANES)):
            tiles = [
                raw[i, :, (3 * g + t) * LANES:(3 * g + t + 1) * LANES].astype(jnp.float32)
                for t in range(3)
            ]
            squares = [t * t for t in tiles]

            def share(t, h):
                low, high = h * HD - t * LANES, (h + 1) * HD - t * LANES
                return jnp.logical_and(lane >= low, lane < high)

            scales = []
            for h in range(4):
                parts = [
                    jnp.where(share(t, h), squares[t], 0.0)
                    for t in range(3)
                    if h * HD < (t + 1) * LANES and (h + 1) * HD > t * LANES
                ]
                total = jnp.sum(functools.reduce(jnp.add, parts), axis=-1, keepdims=True)
                scales.append(lax.rsqrt(total * (1.0 / HD) + 1e-06))
            for t in range(3):
                at = (3 * g + t) * LANES
                scale = jnp.where(share(t, t), scales[t], scales[t + 1])
                normed[i, :, at:at + LANES] = (
                    tiles[t] * scale * tiled[:, t * LANES:(t + 1) * LANES]
                ).astype(jnp.bfloat16)

    loads[2].wait()
    early = rank > owner_ranks[1]
    pl.when(early)(lambda: others(0, lambda o: give_v(o).start()))
    take(gains, gain_sem)
    loads[1].wait()
    normalize(1)
    pl.when(early)(lambda: others(0, lambda o: give_k(o).start()))
    loads[0].wait()
    normalize(0)

    @pl.when(jnp.logical_not(early))
    def _():
        await_ready(0)
        others(0, lambda o: give_v(o).start())
        others(0, lambda o: give_k(o).start())

    pl.when(half == 0)(lambda: others(0, lambda o: give_q(o).start()))
    give_w = pltpu.make_async_remote_copy(
        src_ref=w_hbm,
        dst_ref=w_vmem.at[my_depth],
        send_sem=send_w,
        recv_sem=recv_w,
        device_id={"uly": 1 - uly},
        device_id_type=MESH,
    )

    @pl.when(uly == 1)
    def _():
        pl.semaphore_wait(sib, 1)
        give_w.start()

    await_ready(1)
    others(1, lambda o: give_v(o).start())
    others(1, lambda o: give_k(o).start())
    pl.when(half == 1)(lambda: others(1, lambda o: give_q(o).start()))
    @pl.when(uly == 0)
    def _():
        give_w.start()

    @pl.when(is_owner)
    def _():
        mine = pl.ds(pl.multiple_of(side * shift, LANES), span)
        kbuf[my_rows, :] = normed[1, :, mine]
        vbuf[my_rows, :] = raw[2, :, mine]
        qbuf[q_rows, :] = normed[0, :, mine]
        for l in range(levels):
            @pl.when(l == level)
            def _(l=l):
                take(kbuf.at[pl.ds(0, 3 * rows)], recv_k.at[l])
                take(vbuf.at[pl.ds(0, 3 * rows)], recv_v.at[l])

            @pl.when(l != level)
            def _(l=l):
                take(kbuf.at[pl.ds(0, group)], recv_k.at[l])
                take(vbuf.at[pl.ds(0, group)], recv_v.at[l])
        take(qbuf.at[pl.ds(0, part - rows)], recv_q)

        lane = lax.broadcasted_iota(jnp.int32, (part, 2 * LANES), 1)
        attn[...] = jnp.zeros_like(attn)
        for j in range(len(sides[0])):
            (t0, o0), (t1, o1) = sides[0][j], sides[1][j]
            off = o0 + side * (o1 - o0)
            window = pl.ds(pl.multiple_of((t0 + side * (t1 - t0)) * LANES, LANES), 2 * LANES)
            first = jnp.logical_and(lane >= off, lane < off + HD)
            second = jnp.logical_and(lane >= off + HD, lane < off + 2 * HD)
            query = qbuf[:, window]
            zero = jnp.zeros_like(query)
            query = jnp.concatenate(
                [jnp.where(first, query, zero), jnp.where(second, query, zero)], axis=0
            )
            scores = lax.dot_general(
                query, kbuf[:, window], (((1,), (1,)), ((), ())),
                preferred_element_type=jnp.float32,
            )
            expd = jnp.exp2(scores * (float(HD) ** (-0.5) * LOG2E))
            total = jnp.sum(expd, axis=-1, keepdims=True)
            weighted = jnp.dot(
                expd.astype(jnp.bfloat16), vbuf[:, window], preferred_element_type=jnp.float32
            ) / total
            both = jnp.where(first, weighted[:part], jnp.where(second, weighted[part:], 0.0))
            attn[:, window] += both.astype(jnp.bfloat16)
        for i in range(part // rows):
            b, c = half * (blks // 2) + i // 2, i % 2
            home = jnp.logical_and(b == blk, uly == c)

            @pl.when(jnp.logical_not(home))
            def _(i=i, b=b, c=c):
                pltpu.make_async_remote_copy(
                    src_ref=attn.at[pl.ds(i * rows, rows)],
                    dst_ref=back.at[side],
                    send_sem=send_a,
                    recv_sem=recv_a.at[side],
                    device_id={"blk": b, "uly": c},
                    device_id_type=MESH,
                ).start()

        back[side] = attn[q_rows, :]

    load_w.wait()
    give_w.wait_recv()

    @pl.when(jnp.logical_not(is_owner))
    def _():
        take(back.at[0], recv_a.at[side])

    def project(s):
        return jnp.dot(
            back[s],
            w_vmem[pl.ds(pl.multiple_of(s * shift, LANES), span), :],
            preferred_element_type=jnp.float32,
        )

    acc[...] = project(side)
    take(back.at[0], recv_a.at[1 - side])
    out_ref[...] = (acc[...] + project(1 - side)).astype(out_ref.dtype)

    give_w.wait_send()
    slab = qbuf.at[pl.ds(0, rows)]
    for i in range(3):
        take(slab, send_v)
        take(slab, send_k)
    take(slab, send_q)

    @pl.when(is_owner)
    def _():
        for i in range(part // rows - 1):
            take(slab, send_a)

    @pl.when(jnp.logical_not(is_owner))
    def _():
        for sem in (send_v, send_k, send_q):
            take(slab, sem)


def on_device_gather(blks, query, key, value, q_gain, k_gain, out_weight):
    rows, width = query.shape
    heads = width // HD
    depth, cols = out_weight.shape
    levels = blks // 2
    seq = 2 * blks * rows
    span = pair_windows(width, heads)[0]
    dma = pltpu.SemaphoreType.DMA
    bf16 = jnp.bfloat16
    return pl.pallas_call(
        functools.partial(gather_kernel, blks, heads),
        out_shape=pltpu.VMEM((rows, cols), bf16),
        in_specs=[pl.BlockSpec(memory_space=pltpu.HBM)] * 6,
        out_specs=pl.BlockSpec(memory_space=pltpu.VMEM),
        scratch_shapes=[
            pltpu.VMEM((3, rows, width), bf16),
            pltpu.VMEM((2, 1, HD), jnp.float32),
            pltpu.VMEM((2, rows, width), bf16),
            pltpu.VMEM((seq, span), bf16),
            pltpu.VMEM((seq, span), bf16),
            pltpu.VMEM((seq // 2, span), bf16),
            pltpu.VMEM((seq // 2, span), bf16),
            pltpu.VMEM((2, rows, span), bf16),
            pltpu.VMEM((rows, cols), jnp.float32),
            pltpu.VMEM((width, cols), bf16),
            dma((3,)),
            dma, dma, dma, dma, dma, dma, dma,
            dma((levels,)),
            dma((levels,)),
            dma,
            dma((2,)),
            dma,
            pltpu.SemaphoreType.REGULAR((blks,)),
            pltpu.SemaphoreType.REGULAR,
        ],
        compiler_params=pltpu.CompilerParams(collective_id=0, has_side_effects=True),
    )(query, key, value, q_gain.reshape(1, HD), k_gain.reshape(1, HD), out_weight)


def fits_gather(blks, ulys, width):
    heads = width // HD
    return (
        ulys == 2
        and blks % 4 == 0
        and heads % 4 == 0
        and width % (3 * LANES) == 0
        and (width // LANES) % 2 == 1
        and blks <= heads
    )


def solution(mesh):
    blks, ulys = mesh.shape["blk"], mesh.shape["uly"]
    tokens = P(("grp", "blk", "uly"), None)

    def body(query, *rest):
        if fits_gather(blks, ulys, query.shape[1]):
            return on_device_gather(blks, query, *rest)
        return on_device(blks, ulys, query, *rest)

    return jax.shard_map(
        body,
        mesh=mesh,
        in_specs=(tokens, tokens, tokens, P(), P(), P("uly", None)),
        out_specs=tokens,
        check_vma=False,
    )
```

```python
import functools

import jax
import jax.numpy as jnp
from jax import lax
from jax.experimental import pallas as pl
from jax.experimental.pallas import tpu as pltpu
from jax.sharding import PartitionSpec as P

HD = 96
LANES = 128
CHUNKS = 1
GROUPS = 4
LOG2E = 1.4426950408889634
MESH = pl.DeviceIdType.MESH


def loop(count, body):
    if count <= 32:
        for i in range(count):
            body(i)
    else:
        lax.fori_loop(0, count, lambda i, c: (body(i), c)[1], 0)


def take(ref, sem):
    pltpu.make_async_copy(ref, ref, sem).wait()


def layer_kernel(
    blks, ulys, heads, copies,
    q_hbm, k_hbm, v_hbm, qg_hbm, kg_hbm, w_hbm, out_ref,
    raw, gains, w_vmem, pack, qkv, attn, back, acc,
    load_sem, gain_sem, w_sem, send1, recv1, send2, recv2, send_w, recv_w,
):
    n = blks * ulys
    rows = raw.shape[1]
    owners = heads * copies
    blk, uly = lax.axis_index("blk"), lax.axis_index("uly")
    me = blk * ulys + uly
    seq = n * rows
    block = seq // copies
    chunks = CHUNKS
    chunk = block // chunks
    groups = recv2.shape[0]
    members = heads // groups
    targets = chunk // rows
    depth = w_hbm.shape[0]
    upper = (2 * me) // n

    barrier = pltpu.get_barrier_semaphore()

    def greet(i):
        d = lax.rem(me + n // 2 + i + i // (n // 2), n)
        pl.semaphore_signal(
            barrier, inc=1, device_id={"blk": d // ulys, "uly": d % ulys}, device_id_type=MESH
        )

    loop(n - 1, greet)

    loads = [
        pltpu.make_async_copy(src, raw.at[i], load_sem.at[i])
        for i, src in enumerate((q_hbm, k_hbm, v_hbm))
    ]
    load_gains = [
        pltpu.make_async_copy(src, gains.at[i], gain_sem)
        for i, src in enumerate((qg_hbm, kg_hbm))
    ]
    for one in loads + load_gains:
        one.start()

    def mirror(d):
        plane = d // 4
        return d + (plane % 2) * (3 - 2 * (d % 4))

    def owner_device(o):
        return mirror(o * n // owners)

    spot = mirror(me)
    slot = (spot * owners + n - 1) // n
    is_owner = jnp.logical_and(slot < owners, (slot * n) // owners == spot)
    slot = jnp.minimum(slot, owners - 1)

    my_depth = pl.ds(pl.multiple_of(uly * depth, depth), depth)
    load_w = pltpu.make_async_copy(w_hbm, w_vmem.at[my_depth], w_sem)
    load_w.start()

    pad = jnp.zeros((rows, LANES - HD), jnp.bfloat16)
    take(gains, gain_sem)
    for i in range(2):
        loads[i].wait()
        gain = gains[i]
        for h in range(heads):
            x = raw[i, :, h * HD:(h + 1) * HD].astype(jnp.float32)
            scale = lax.rsqrt(jnp.mean(x * x, axis=-1, keepdims=True) + 1e-06)
            normed = (x * scale * gain).astype(jnp.bfloat16)
            pack[h, :, i * LANES:(i + 1) * LANES] = jnp.concatenate([normed, pad], axis=1)
    loads[2].wait()
    for h in range(heads):
        x = raw[2, :, h * HD:(h + 1) * HD]
        pack[h, :, 2 * LANES:3 * LANES] = jnp.concatenate([x, pad], axis=1)

    pl.semaphore_wait(barrier, n - 1)

    my_rows = pl.ds(pl.multiple_of(me * rows, rows), rows)

    def send_of(o):
        d = owner_device(o)
        return d, pltpu.make_async_remote_copy(
            src_ref=pack.at[o // copies],
            dst_ref=qkv.at[my_rows],
            send_sem=send1,
            recv_sem=recv1,
            device_id={"blk": d // ulys, "uly": d % ulys},
            device_id_type=MESH,
        )

    def send(i):
        d, copy = send_of(owners - 1 - i + upper * (2 * i + 1 - owners))

        @pl.when(d != me)
        def _():
            copy.start()

    loop(owners, send)

    give_w = pltpu.make_async_remote_copy(
        src_ref=w_hbm,
        dst_ref=w_vmem.at[my_depth],
        send_sem=send_w,
        recv_sem=recv_w,
        device_id={"blk": blk, "uly": 1 - uly},
        device_id_type=MESH,
    )
    give_w.start()

    @pl.when(is_owner)
    def _():
        head = slot // copies
        part = slot % copies
        qkv[my_rows, :] = pack[head]

        take(qkv.at[pl.ds(0, (n - 1) * rows)], recv1)
        score_scale = float(HD) ** (-0.5)

        def step(query, j, carry):
            weighted, total = carry
            here = pl.ds(j * block, block)
            keys = qkv[here, LANES:2 * LANES]
            values = qkv[here, 2 * LANES:3 * LANES]
            scores = lax.dot_general(
                query, keys, (((1,), (1,)), ((), ())), preferred_element_type=jnp.float32
            ) * score_scale
            expd = jnp.exp(scores)
            total = total + jnp.sum(expd, axis=-1, keepdims=True)
            weighted = weighted + jnp.dot(
                expd.astype(jnp.bfloat16), values, preferred_element_type=jnp.float32
            )
            return weighted, total

        def result_copies(c):
            for k in range(targets):
                i = targets - 1 - k + upper * (2 * k + 1 - targets)
                d = (part * chunks + c) * targets + i
                src = attn.at[pl.ds(pl.multiple_of((c * targets + i) * rows, rows), rows)]
                yield (
                    d == me,
                    functools.partial(
                        pltpu.make_async_copy, src, back.at[head], recv2.at[head // members]
                    ),
                    pltpu.make_async_remote_copy(
                        src_ref=src,
                        dst_ref=back.at[head],
                        send_sem=send2,
                        recv_sem=recv2.at[head // members],
                        device_id={"blk": d // ulys, "uly": d % ulys},
                        device_id_type=MESH,
                    ),
                )

        for k in range(chunks):
            c = chunks - 1 - k + upper * (2 * k + 1 - chunks)
            at = part * block + c * chunk
            query = qkv[pl.ds(pl.multiple_of(at, chunk), chunk), 0:LANES]
            carry = (jnp.zeros((chunk, LANES), jnp.float32), jnp.zeros((chunk, 1), jnp.float32))
            if copies == 1:
                weighted, total = step(query, 0, carry)
            else:
                weighted, total = lax.fori_loop(
                    0, copies, functools.partial(lambda q, j, c: step(q, j, c), query), carry
                )
            attn[pl.ds(pl.multiple_of(c * chunk, chunk), chunk), :] = (weighted / total).astype(jnp.bfloat16)
            for home, local, remote in result_copies(c):
                pl.when(home)(lambda local=local: local().start())
                pl.when(jnp.logical_not(home))(remote.start)

    load_w.wait()
    give_w.wait_recv()
    first = (me * groups) // n
    for i in range(groups):
        g = lax.rem(first + i * (1 - 2 * upper) + groups, groups)
        take(back.at[pl.ds(g * members, members)], recv2.at[g])
        for j in range(members):
            h = g * members + j
            term = jnp.dot(
                back[h, :, 0:HD],
                w_vmem[pl.ds(pl.multiple_of(h * HD, HD), HD), :],
                preferred_element_type=jnp.float32,
            )
            if i == 0 and j == 0:
                acc[...] = term
            elif i < groups - 1 or j < members - 1:
                acc[...] += term
            else:
                out_ref[...] = (acc[...] + term).astype(out_ref.dtype)

    give_w.wait_send()
    for i in range(copies - 1):
        take(pack, send1)

    @pl.when(is_owner)
    def _():
        take(pack.at[pl.ds(0, heads - 1)], send1)
        at_home = (slot % copies) * block == (me * rows) // block * block
        pl.when(at_home)(lambda: take(attn.at[pl.ds(0, block - rows)], send2))
        pl.when(jnp.logical_not(at_home))(lambda: take(attn, send2))

    @pl.when(jnp.logical_not(is_owner))
    def _():
        take(pack, send1)


def on_device(blks, ulys, query, key, value, q_gain, k_gain, out_weight):
    rows, width = query.shape
    heads = width // HD
    n = blks * ulys
    copies = 1
    while heads * copies * 2 <= n:
        copies *= 2
    owners = heads * copies
    depth, cols = out_weight.shape
    seq = n * rows
    block = seq // copies
    dma = pltpu.SemaphoreType.DMA
    return pl.pallas_call(
        functools.partial(layer_kernel, blks, ulys, heads, copies),
        out_shape=pltpu.VMEM((rows, cols), jnp.bfloat16),
        in_specs=[pl.BlockSpec(memory_space=pltpu.HBM)] * 6,
        out_specs=pl.BlockSpec(memory_space=pltpu.VMEM),
        scratch_shapes=[
            pltpu.VMEM((3, rows, width), jnp.bfloat16),
            pltpu.VMEM((2, 1, HD), jnp.float32),
            pltpu.VMEM((width, cols), jnp.bfloat16),
            pltpu.VMEM((heads, rows, 3 * LANES), jnp.bfloat16),
            pltpu.VMEM((seq, 3 * LANES), jnp.bfloat16),
            pltpu.VMEM((block, LANES), jnp.bfloat16),
            pltpu.VMEM((heads, rows, LANES), jnp.bfloat16),
            pltpu.VMEM((rows, cols), jnp.float32),
            dma((3,)),
            dma,
            dma,
            dma,
            dma,
            dma,
            dma((GROUPS,)),
            dma,
            dma,
        ],
        compiler_params=pltpu.CompilerParams(collective_id=0, has_side_effects=True),
    )(query, key, value, q_gain.reshape(1, HD), k_gain.reshape(1, HD), out_weight)


def pair_windows(width, heads):
    tiles = width // LANES
    span = (tiles + 1) // 2
    half = heads // 2
    sides = []
    for side in range(2):
        base = side * (tiles - span)
        one = []
        for j in range(half // 2):
            lane = (side * half + 2 * j) * HD
            tile = lane // LANES
            one.append((tile - base, lane - tile * LANES))
        sides.append(one)
    return span * LANES, (tiles - span) * LANES, sides


def gather_kernel(
    blks, heads,
    q_hbm, k_hbm, v_hbm, qg_hbm, kg_hbm, w_hbm, out_ref,
    raw, gains, normed, kbuf, vbuf, qbuf, attn, back, acc, w_vmem,
    load_sem, gain_sem, w_sem, send_v, send_k, send_q, send_a, send_w,
    recv_v, recv_k, recv_q, recv_a, recv_w, ready,
):
    levels = blks // 2
    rows, width = raw.shape[1:]
    span, shift, sides = pair_windows(width, heads)
    group = 4 * rows
    half_levels = levels // 2
    part = half_levels * group
    blk, uly = lax.axis_index("blk"), lax.axis_index("uly")
    level, side = blk // 2, blk % 2
    me = blk * 2 + uly
    half = level // half_levels
    owners = [(h, s, (half_levels - 1 + h) * 2 + s) for h in range(2) for s in range(2)]
    is_owner = functools.reduce(
        jnp.logical_or, [jnp.logical_and(uly == 1, blk == b) for _, _, b in owners]
    )
    my_rows = pl.ds(pl.multiple_of(me * rows, rows), rows)
    depth = w_hbm.shape[0]
    my_depth = pl.ds(pl.multiple_of(uly * depth, depth), depth)

    load_gains = [
        pltpu.make_async_copy(src, gains.at[i], gain_sem)
        for i, src in enumerate((qg_hbm, kg_hbm))
    ]
    loads = [
        pltpu.make_async_copy(src, raw.at[i], load_sem.at[i])
        for i, src in enumerate((q_hbm, k_hbm, v_hbm))
    ]
    for one in (loads[2], loads[1], *load_gains, loads[0]):
        one.start()

    barrier = pltpu.get_barrier_semaphore()
    late = half == 1
    for d in range(2 * blks):
        b, c = d // 2, d % 2
        cond = jnp.logical_or(
            jnp.logical_and(blk == b, uly == 1 - c),
            jnp.logical_and(is_owner, me != d if b >= blks // 2 else jnp.logical_and(me != d, jnp.logical_not(late))),
        )
        if c == 1 and b in [o[2] for o in owners[2:]]:
            cond = jnp.logical_or(cond, jnp.logical_not(late))

        @pl.when(cond)
        def _(b=b, c=c):
            pl.semaphore_signal(
                barrier, inc=1, device_id={"blk": b, "uly": c}, device_id_type=MESH
            )

    load_w = pltpu.make_async_copy(w_hbm, w_vmem.at[my_depth], w_sem)
    load_w.start()

    owner_here = functools.reduce(jnp.logical_or, [blk == b for _, _, b in owners])
    heard = 3 + 2 * half - owner_here.astype(jnp.int32)
    heard += jnp.where(jnp.logical_and(is_owner, late), blks - 2, 0)
    pl.semaphore_wait(barrier, heard)

    @pl.when(jnp.logical_and(is_owner, late))
    def _():
        for d in range(blks):
            pl.semaphore_signal(
                ready.at[side], inc=1, device_id={"blk": d // 2, "uly": d % 2}, device_id_type=MESH
            )

    def give(src, dst, owner, send, recv):
        h, s = owner
        return pltpu.make_async_remote_copy(
            src_ref=src.at[:, pl.ds(pl.multiple_of(s * shift, LANES), span)],
            dst_ref=dst,
            send_sem=send,
            recv_sem=recv,
            device_id={"blk": (half_levels - 1 + h) * 2 + s, "uly": 1},
            device_id_type=MESH,
        )

    def give_v(owner):
        return give(raw.at[2], vbuf.at[my_rows], owner, send_v, recv_v.at[level])

    def give_k(owner):
        return give(normed.at[1], kbuf.at[my_rows], owner, send_k, recv_k.at[level])

    q_rows = pl.ds(pl.multiple_of((me - half * (2 * blks // 2)) * rows, rows), rows)

    def give_q(owner):
        return give(normed.at[0], qbuf.at[q_rows], owner, send_q, recv_q)

    def others(h, body):
        body((h, 1 - side))
        mine = jnp.logical_and(uly == 1, blk == (half_levels - 1 + h) * 2 + side)
        pl.when(jnp.logical_not(mine))(lambda: body((h, side)))

    def normalize(i):
        tiled = jnp.concatenate([gains[i]] * 4, axis=1)
        lane = lax.broadcasted_iota(jnp.int32, (rows, LANES), 1)
        for g in range(width // (3 * LANES)):
            tiles = [
                raw[i, :, (3 * g + t) * LANES:(3 * g + t + 1) * LANES].astype(jnp.float32)
                for t in range(3)
            ]
            squares = [t * t for t in tiles]

            def share(t, h):
                low, high = h * HD - t * LANES, (h + 1) * HD - t * LANES
                return jnp.logical_and(lane >= low, lane < high)

            scales = []
            for h in range(4):
                parts = [
                    jnp.where(share(t, h), squares[t], 0.0)
                    for t in range(3)
                    if h * HD < (t + 1) * LANES and (h + 1) * HD > t * LANES
                ]
                total = jnp.sum(functools.reduce(jnp.add, parts), axis=-1, keepdims=True)
                scales.append(lax.rsqrt(total * (1.0 / HD) + 1e-06))
            for t in range(3):
                at = (3 * g + t) * LANES
                scale = jnp.where(share(t, t), scales[t], scales[t + 1])
                normed[i, :, at:at + LANES] = (
                    tiles[t] * scale * tiled[:, t * LANES:(t + 1) * LANES]
                ).astype(jnp.bfloat16)

    loads[2].wait()
    others(0, lambda o: give_v(o).start())
    take(gains, gain_sem)
    loads[1].wait()
    normalize(1)
    others(0, lambda o: give_k(o).start())
    loads[0].wait()
    normalize(0)
    pl.when(half == 0)(lambda: others(0, lambda o: give_q(o).start()))

    @pl.when(jnp.logical_not(late))
    def _():
        for i in range(2):
            pl.semaphore_wait(ready.at[i], 1)

    others(1, lambda o: give_v(o).start())
    others(1, lambda o: give_k(o).start())
    pl.when(half == 1)(lambda: others(1, lambda o: give_q(o).start()))
    give_w = pltpu.make_async_remote_copy(
        src_ref=w_hbm,
        dst_ref=w_vmem.at[my_depth],
        send_sem=send_w,
        recv_sem=recv_w,
        device_id={"uly": 1 - uly},
        device_id_type=MESH,
    )

    give_w.start()

    @pl.when(is_owner)
    def _():
        mine = pl.ds(pl.multiple_of(side * shift, LANES), span)
        kbuf[my_rows, :] = normed[1, :, mine]
        vbuf[my_rows, :] = raw[2, :, mine]
        qbuf[q_rows, :] = normed[0, :, mine]
        for l in range(levels):
            @pl.when(l == level)
            def _(l=l):
                take(kbuf.at[pl.ds(0, 3 * rows)], recv_k.at[l])
                take(vbuf.at[pl.ds(0, 3 * rows)], recv_v.at[l])

            @pl.when(l != level)
            def _(l=l):
                take(kbuf.at[pl.ds(0, group)], recv_k.at[l])
                take(vbuf.at[pl.ds(0, group)], recv_v.at[l])
        take(qbuf.at[pl.ds(0, part - rows)], recv_q)

        lane = lax.broadcasted_iota(jnp.int32, (part, 2 * LANES), 1)
        attn[...] = jnp.zeros_like(attn)
        for j in range(len(sides[0])):
            (t0, o0), (t1, o1) = sides[0][j], sides[1][j]
            off = o0 + side * (o1 - o0)
            window = pl.ds(pl.multiple_of((t0 + side * (t1 - t0)) * LANES, LANES), 2 * LANES)
            first = jnp.logical_and(lane >= off, lane < off + HD)
            second = jnp.logical_and(lane >= off + HD, lane < off + 2 * HD)
            query = qbuf[:, window]
            zero = jnp.zeros_like(query)
            query = jnp.concatenate(
                [jnp.where(first, query, zero), jnp.where(second, query, zero)], axis=0
            )
            scores = lax.dot_general(
                query, kbuf[:, window], (((1,), (1,)), ((), ())),
                preferred_element_type=jnp.float32,
            )
            expd = jnp.exp2(scores * (float(HD) ** (-0.5) * LOG2E))
            total = jnp.sum(expd, axis=-1, keepdims=True)
            weighted = jnp.dot(
                expd.astype(jnp.bfloat16), vbuf[:, window], preferred_element_type=jnp.float32
            ) / total
            both = jnp.where(first, weighted[:part], jnp.where(second, weighted[part:], 0.0))
            attn[:, window] += both.astype(jnp.bfloat16)
        for i in range(part // rows):
            b, c = half * (blks // 2) + i // 2, i % 2
            home = jnp.logical_and(b == blk, uly == c)

            @pl.when(jnp.logical_not(home))
            def _(i=i, b=b, c=c):
                pltpu.make_async_remote_copy(
                    src_ref=attn.at[pl.ds(i * rows, rows)],
                    dst_ref=back.at[side],
                    send_sem=send_a,
                    recv_sem=recv_a.at[side],
                    device_id={"blk": b, "uly": c},
                    device_id_type=MESH,
                ).start()

        back[side] = attn[q_rows, :]

    load_w.wait()
    give_w.wait_recv()

    @pl.when(jnp.logical_not(is_owner))
    def _():
        take(back.at[0], recv_a.at[side])

    def project(s):
        return jnp.dot(
            back[s],
            w_vmem[pl.ds(pl.multiple_of(s * shift, LANES), span), :],
            preferred_element_type=jnp.float32,
        )

    acc[...] = project(side)
    take(back.at[0], recv_a.at[1 - side])
    out_ref[...] = (acc[...] + project(1 - side)).astype(out_ref.dtype)

    give_w.wait_send()
    slab = qbuf.at[pl.ds(0, rows)]
    for i in range(3):
        take(slab, send_v)
        take(slab, send_k)
    take(slab, send_q)

    @pl.when(is_owner)
    def _():
        for i in range(part // rows - 1):
            take(slab, send_a)

    @pl.when(jnp.logical_not(is_owner))
    def _():
        for sem in (send_v, send_k, send_q):
            take(slab, sem)


def on_device_gather(blks, query, key, value, q_gain, k_gain, out_weight):
    rows, width = query.shape
    heads = width // HD
    depth, cols = out_weight.shape
    levels = blks // 2
    seq = 2 * blks * rows
    span = pair_windows(width, heads)[0]
    dma = pltpu.SemaphoreType.DMA
    bf16 = jnp.bfloat16
    return pl.pallas_call(
        functools.partial(gather_kernel, blks, heads),
        out_shape=pltpu.VMEM((rows, cols), bf16),
        in_specs=[pl.BlockSpec(memory_space=pltpu.HBM)] * 6,
        out_specs=pl.BlockSpec(memory_space=pltpu.VMEM),
        scratch_shapes=[
            pltpu.VMEM((3, rows, width), bf16),
            pltpu.VMEM((2, 1, HD), jnp.float32),
            pltpu.VMEM((2, rows, width), bf16),
            pltpu.VMEM((seq, span), bf16),
            pltpu.VMEM((seq, span), bf16),
            pltpu.VMEM((seq // 2, span), bf16),
            pltpu.VMEM((seq // 2, span), bf16),
            pltpu.VMEM((2, rows, span), bf16),
            pltpu.VMEM((rows, cols), jnp.float32),
            pltpu.VMEM((width, cols), bf16),
            dma((3,)),
            dma, dma, dma, dma, dma, dma, dma,
            dma((levels,)),
            dma((levels,)),
            dma,
            dma((2,)),
            dma,
            pltpu.SemaphoreType.REGULAR((2,)),
        ],
        compiler_params=pltpu.CompilerParams(collective_id=0, has_side_effects=True),
    )(query, key, value, q_gain.reshape(1, HD), k_gain.reshape(1, HD), out_weight)


def fits_gather(blks, ulys, width):
    heads = width // HD
    return (
        ulys == 2
        and blks % 4 == 0
        and heads % 4 == 0
        and width % (3 * LANES) == 0
        and (width // LANES) % 2 == 1
        and blks <= heads
    )


def solution(mesh):
    blks, ulys = mesh.shape["blk"], mesh.shape["uly"]
    tokens = P(("grp", "blk", "uly"), None)

    def body(query, *rest):
        if fits_gather(blks, ulys, query.shape[1]):
            return on_device_gather(blks, query, *rest)
        return on_device(blks, ulys, query, *rest)

    return jax.shard_map(
        body,
        mesh=mesh,
        in_specs=(tokens, tokens, tokens, P(), P(), P("uly", None)),
        out_specs=tokens,
        check_vma=False,
    )
```

```python
import functools

import jax
import jax.numpy as jnp
from jax import lax
from jax.experimental import pallas as pl
from jax.experimental.pallas import tpu as pltpu
from jax.sharding import PartitionSpec as P

HD = 96
LANES = 128
CHUNKS = 1
GROUPS = 4
LOG2E = 1.4426950408889634
MESH = pl.DeviceIdType.MESH


def loop(count, body):
    if count <= 32:
        for i in range(count):
            body(i)
    else:
        lax.fori_loop(0, count, lambda i, c: (body(i), c)[1], 0)


def take(ref, sem):
    pltpu.make_async_copy(ref, ref, sem).wait()


def layer_kernel(
    blks, ulys, heads, copies,
    q_hbm, k_hbm, v_hbm, qg_hbm, kg_hbm, w_hbm, out_ref,
    raw, gains, w_vmem, pack, qkv, attn, back, acc,
    load_sem, gain_sem, w_sem, send1, recv1, send2, recv2, send_w, recv_w,
):
    n = blks * ulys
    rows = raw.shape[1]
    owners = heads * copies
    blk, uly = lax.axis_index("blk"), lax.axis_index("uly")
    me = blk * ulys + uly
    seq = n * rows
    block = seq // copies
    chunks = CHUNKS
    chunk = block // chunks
    groups = recv2.shape[0]
    members = heads // groups
    targets = chunk // rows
    depth = w_hbm.shape[0]
    upper = (2 * me) // n

    barrier = pltpu.get_barrier_semaphore()

    def greet(i):
        d = lax.rem(me + n // 2 + i + i // (n // 2), n)
        pl.semaphore_signal(
            barrier, inc=1, device_id={"blk": d // ulys, "uly": d % ulys}, device_id_type=MESH
        )

    loop(n - 1, greet)

    loads = [
        pltpu.make_async_copy(src, raw.at[i], load_sem.at[i])
        for i, src in enumerate((q_hbm, k_hbm, v_hbm))
    ]
    load_gains = [
        pltpu.make_async_copy(src, gains.at[i], gain_sem)
        for i, src in enumerate((qg_hbm, kg_hbm))
    ]
    for one in loads + load_gains:
        one.start()

    def mirror(d):
        plane = d // 4
        return d + (plane % 2) * (3 - 2 * (d % 4))

    def owner_device(o):
        return mirror(o * n // owners)

    spot = mirror(me)
    slot = (spot * owners + n - 1) // n
    is_owner = jnp.logical_and(slot < owners, (slot * n) // owners == spot)
    slot = jnp.minimum(slot, owners - 1)

    my_depth = pl.ds(pl.multiple_of(uly * depth, depth), depth)
    load_w = pltpu.make_async_copy(w_hbm, w_vmem.at[my_depth], w_sem)
    load_w.start()

    pad = jnp.zeros((rows, LANES - HD), jnp.bfloat16)
    take(gains, gain_sem)
    for i in range(2):
        loads[i].wait()
        gain = gains[i]
        for h in range(heads):
            x = raw[i, :, h * HD:(h + 1) * HD].astype(jnp.float32)
            scale = lax.rsqrt(jnp.mean(x * x, axis=-1, keepdims=True) + 1e-06)
            normed = (x * scale * gain).astype(jnp.bfloat16)
            pack[h, :, i * LANES:(i + 1) * LANES] = jnp.concatenate([normed, pad], axis=1)
    loads[2].wait()
    for h in range(heads):
        x = raw[2, :, h * HD:(h + 1) * HD]
        pack[h, :, 2 * LANES:3 * LANES] = jnp.concatenate([x, pad], axis=1)

    pl.semaphore_wait(barrier, n - 1)

    my_rows = pl.ds(pl.multiple_of(me * rows, rows), rows)

    def send_of(o):
        d = owner_device(o)
        return d, pltpu.make_async_remote_copy(
            src_ref=pack.at[o // copies],
            dst_ref=qkv.at[my_rows],
            send_sem=send1,
            recv_sem=recv1,
            device_id={"blk": d // ulys, "uly": d % ulys},
            device_id_type=MESH,
        )

    def send(i):
        d, copy = send_of(owners - 1 - i + upper * (2 * i + 1 - owners))

        @pl.when(d != me)
        def _():
            copy.start()

    loop(owners, send)

    give_w = pltpu.make_async_remote_copy(
        src_ref=w_hbm,
        dst_ref=w_vmem.at[my_depth],
        send_sem=send_w,
        recv_sem=recv_w,
        device_id={"blk": blk, "uly": 1 - uly},
        device_id_type=MESH,
    )
    give_w.start()

    @pl.when(is_owner)
    def _():
        head = slot // copies
        part = slot % copies
        qkv[my_rows, :] = pack[head]

        take(qkv.at[pl.ds(0, (n - 1) * rows)], recv1)
        score_scale = float(HD) ** (-0.5)

        def step(query, j, carry):
            weighted, total = carry
            here = pl.ds(j * block, block)
            keys = qkv[here, LANES:2 * LANES]
            values = qkv[here, 2 * LANES:3 * LANES]
            scores = lax.dot_general(
                query, keys, (((1,), (1,)), ((), ())), preferred_element_type=jnp.float32
            ) * score_scale
            expd = jnp.exp(scores)
            total = total + jnp.sum(expd, axis=-1, keepdims=True)
            weighted = weighted + jnp.dot(
                expd.astype(jnp.bfloat16), values, preferred_element_type=jnp.float32
            )
            return weighted, total

        def result_copies(c):
            for k in range(targets):
                i = targets - 1 - k + upper * (2 * k + 1 - targets)
                d = (part * chunks + c) * targets + i
                src = attn.at[pl.ds(pl.multiple_of((c * targets + i) * rows, rows), rows)]
                yield (
                    d == me,
                    functools.partial(
                        pltpu.make_async_copy, src, back.at[head], recv2.at[head // members]
                    ),
                    pltpu.make_async_remote_copy(
                        src_ref=src,
                        dst_ref=back.at[head],
                        send_sem=send2,
                        recv_sem=recv2.at[head // members],
                        device_id={"blk": d // ulys, "uly": d % ulys},
                        device_id_type=MESH,
                    ),
                )

        for k in range(chunks):
            c = chunks - 1 - k + upper * (2 * k + 1 - chunks)
            at = part * block + c * chunk
            query = qkv[pl.ds(pl.multiple_of(at, chunk), chunk), 0:LANES]
            carry = (jnp.zeros((chunk, LANES), jnp.float32), jnp.zeros((chunk, 1), jnp.float32))
            if copies == 1:
                weighted, total = step(query, 0, carry)
            else:
                weighted, total = lax.fori_loop(
                    0, copies, functools.partial(lambda q, j, c: step(q, j, c), query), carry
                )
            attn[pl.ds(pl.multiple_of(c * chunk, chunk), chunk), :] = (weighted / total).astype(jnp.bfloat16)
            for home, local, remote in result_copies(c):
                pl.when(home)(lambda local=local: local().start())
                pl.when(jnp.logical_not(home))(remote.start)

    load_w.wait()
    give_w.wait_recv()
    first = (me * groups) // n
    for i in range(groups):
        g = lax.rem(first + i * (1 - 2 * upper) + groups, groups)
        take(back.at[pl.ds(g * members, members)], recv2.at[g])
        for j in range(members):
            h = g * members + j
            term = jnp.dot(
                back[h, :, 0:HD],
                w_vmem[pl.ds(pl.multiple_of(h * HD, HD), HD), :],
                preferred_element_type=jnp.float32,
            )
            if i == 0 and j == 0:
                acc[...] = term
            elif i < groups - 1 or j < members - 1:
                acc[...] += term
            else:
                out_ref[...] = (acc[...] + term).astype(out_ref.dtype)

    give_w.wait_send()
    for i in range(copies - 1):
        take(pack, send1)

    @pl.when(is_owner)
    def _():
        take(pack.at[pl.ds(0, heads - 1)], send1)
        at_home = (slot % copies) * block == (me * rows) // block * block
        pl.when(at_home)(lambda: take(attn.at[pl.ds(0, block - rows)], send2))
        pl.when(jnp.logical_not(at_home))(lambda: take(attn, send2))

    @pl.when(jnp.logical_not(is_owner))
    def _():
        take(pack, send1)


def on_device(blks, ulys, query, key, value, q_gain, k_gain, out_weight):
    rows, width = query.shape
    heads = width // HD
    n = blks * ulys
    copies = 1
    while heads * copies * 2 <= n:
        copies *= 2
    owners = heads * copies
    depth, cols = out_weight.shape
    seq = n * rows
    block = seq // copies
    dma = pltpu.SemaphoreType.DMA
    return pl.pallas_call(
        functools.partial(layer_kernel, blks, ulys, heads, copies),
        out_shape=pltpu.VMEM((rows, cols), jnp.bfloat16),
        in_specs=[pl.BlockSpec(memory_space=pltpu.HBM)] * 6,
        out_specs=pl.BlockSpec(memory_space=pltpu.VMEM),
        scratch_shapes=[
            pltpu.VMEM((3, rows, width), jnp.bfloat16),
            pltpu.VMEM((2, 1, HD), jnp.float32),
            pltpu.VMEM((width, cols), jnp.bfloat16),
            pltpu.VMEM((heads, rows, 3 * LANES), jnp.bfloat16),
            pltpu.VMEM((seq, 3 * LANES), jnp.bfloat16),
            pltpu.VMEM((block, LANES), jnp.bfloat16),
            pltpu.VMEM((heads, rows, LANES), jnp.bfloat16),
            pltpu.VMEM((rows, cols), jnp.float32),
            dma((3,)),
            dma,
            dma,
            dma,
            dma,
            dma,
            dma((GROUPS,)),
            dma,
            dma,
        ],
        compiler_params=pltpu.CompilerParams(collective_id=0, has_side_effects=True),
    )(query, key, value, q_gain.reshape(1, HD), k_gain.reshape(1, HD), out_weight)


def gather_kernel(
    blks, heads,
    q_hbm, k_hbm, v_hbm, qg_hbm, kg_hbm, w_hbm, out_ref,
    raw, gains, k_four, kv_two, q_all, kbuf, vbuf, tbuf, qbuf, four, two, back4, back2, acc, w_vmem,
    load_sem, gain_sem, w_sem, send_kv, send_q, send4, send2, send_w,
    recv_kv, recv_q, recv4, recv2, recv_w, ready,
):
    levels = blks // 2
    rows, width = raw.shape[1:]
    wide, pair = 4 * HD, 2 * HD
    last = width - wide
    group = 4 * rows
    half_levels = levels // 2
    part = half_levels * group
    blk, uly = lax.axis_index("blk"), lax.axis_index("uly")
    level, side = blk // 2, blk % 2
    me = blk * 2 + uly
    half = level // half_levels
    owners = [(h, s, (half_levels - 1 + h) * 2 + s) for h in range(2) for s in range(2)]
    is_owner = functools.reduce(
        jnp.logical_or, [jnp.logical_and(uly == 1, blk == b) for _, _, b in owners]
    )
    my_rows = pl.ds(pl.multiple_of(me * rows, rows), rows)
    depth = w_hbm.shape[0]
    my_depth = pl.ds(pl.multiple_of(uly * depth, depth), depth)

    load_gains = [
        pltpu.make_async_copy(src, gains.at[i], gain_sem)
        for i, src in enumerate((qg_hbm, kg_hbm))
    ]
    loads = [
        pltpu.make_async_copy(src, raw.at[i], load_sem.at[i])
        for i, src in enumerate((q_hbm, k_hbm, v_hbm))
    ]
    for one in (loads[2], loads[1], *load_gains, loads[0]):
        one.start()

    barrier = pltpu.get_barrier_semaphore()
    late = half == 1
    for d in range(2 * blks):
        b, c = d // 2, d % 2
        cond = jnp.logical_or(
            jnp.logical_and(blk == b, uly == 1 - c),
            jnp.logical_and(is_owner, me != d if b >= blks // 2 else jnp.logical_and(me != d, jnp.logical_not(late))),
        )
        if c == 1 and b in [o[2] for o in owners[2:]]:
            cond = jnp.logical_or(cond, jnp.logical_not(late))

        @pl.when(cond)
        def _(b=b, c=c):
            pl.semaphore_signal(
                barrier, inc=1, device_id={"blk": b, "uly": c}, device_id_type=MESH
            )

    load_w = pltpu.make_async_copy(w_hbm, w_vmem.at[my_depth], w_sem)
    load_w.start()

    owner_here = functools.reduce(jnp.logical_or, [blk == b for _, _, b in owners])
    heard = 3 + 2 * half - owner_here.astype(jnp.int32)
    heard += jnp.where(jnp.logical_and(is_owner, late), blks - 2, 0)
    pl.semaphore_wait(barrier, heard)

    @pl.when(jnp.logical_and(is_owner, late))
    def _():
        for d in range(blks):
            pl.semaphore_signal(
                ready.at[side], inc=1, device_id={"blk": d // 2, "uly": d % 2}, device_id_type=MESH
            )

    def give(src, dst, owner, send, recv):
        h, s = owner
        return pltpu.make_async_remote_copy(
            src_ref=src,
            dst_ref=dst,
            send_sem=send,
            recv_sem=recv,
            device_id={"blk": (half_levels - 1 + h) * 2 + s, "uly": 1},
            device_id_type=MESH,
        )

    def v_four(s):
        return raw.at[2, :, pl.ds(pl.multiple_of(s * last, LANES), wide)]

    def give_v(owner):
        return give(v_four(owner[1]), vbuf.at[my_rows], owner, send_kv, recv_kv.at[0, level])

    def give_k(owner):
        return give(k_four.at[owner[1]], kbuf.at[my_rows], owner, send_kv, recv_kv.at[1, level])

    def give_two(owner):
        return give(kv_two.at[owner[1]], tbuf.at[my_rows], owner, send_kv, recv_kv.at[2, level])

    q_rows = pl.ds(pl.multiple_of((me - half * (2 * blks // 2)) * rows, rows), rows)

    def give_q(owner):
        return give(q_all.at[owner[1]], qbuf.at[q_rows], owner, send_q, recv_q)

    def others(h, body):
        body((h, 1 - side))
        mine = jnp.logical_and(uly == 1, blk == (half_levels - 1 + h) * 2 + side)
        pl.when(jnp.logical_not(mine))(lambda: body((h, side)))

    def normalize(i, g):
        tiled = jnp.concatenate([gains[i]] * 4, axis=1)
        lane = lax.broadcasted_iota(jnp.int32, (rows, LANES), 1)
        tiles = [
            raw[i, :, (3 * g + t) * LANES:(3 * g + t + 1) * LANES].astype(jnp.float32)
            for t in range(3)
        ]
        squares = [t * t for t in tiles]

        def share(t, h):
            low, high = h * HD - t * LANES, (h + 1) * HD - t * LANES
            return jnp.logical_and(lane >= low, lane < high)

        scales = []
        for h in range(4):
            parts = [
                jnp.where(share(t, h), squares[t], 0.0)
                for t in range(3)
                if h * HD < (t + 1) * LANES and (h + 1) * HD > t * LANES
            ]
            total = jnp.sum(functools.reduce(jnp.add, parts), axis=-1, keepdims=True)
            scales.append(lax.rsqrt(total * (1.0 / HD) + 1e-06))
        return jnp.concatenate(
            [
                tiles[t]
                * jnp.where(share(t, t), scales[t], scales[t + 1])
                * tiled[:, t * LANES:(t + 1) * LANES]
                for t in range(3)
            ],
            axis=1,
        ).astype(jnp.bfloat16)

    loads[2].wait()
    others(0, lambda o: give_v(o).start())
    take(gains, gain_sem)
    loads[1].wait()
    for s in range(2):
        k_four[s] = normalize(1, 2 * s)
    others(0, lambda o: give_k(o).start())
    middle = normalize(1, 1)
    for s in range(2):
        kv_two[s] = jnp.concatenate(
            [middle[:, s * pair:(s + 1) * pair], raw[2, :, wide + s * pair:wide + (s + 1) * pair]],
            axis=1,
        )
    others(0, lambda o: give_two(o).start())
    loads[0].wait()
    middle = normalize(0, 1)
    pad = jnp.zeros((rows, 2 * LANES - pair), jnp.bfloat16)
    for s in range(2):
        q_all[s, :, 0:wide] = normalize(0, 2 * s)
        q_all[s, :, wide:] = jnp.concatenate([middle[:, s * pair:(s + 1) * pair], pad], axis=1)
    pl.when(half == 0)(lambda: others(0, lambda o: give_q(o).start()))

    @pl.when(jnp.logical_not(late))
    def _():
        for i in range(2):
            pl.semaphore_wait(ready.at[i], 1)

    for one in (give_v, give_k, give_two):
        others(1, lambda o, one=one: one(o).start())
    pl.when(half == 1)(lambda: others(1, lambda o: give_q(o).start()))
    give_w = pltpu.make_async_remote_copy(
        src_ref=w_hbm,
        dst_ref=w_vmem.at[my_depth],
        send_sem=send_w,
        recv_sem=recv_w,
        device_id={"uly": 1 - uly},
        device_id_type=MESH,
    )

    give_w.start()

    @pl.when(is_owner)
    def _():
        kbuf[my_rows, :] = k_four[side]
        vbuf[my_rows, :] = v_four(side)[...]
        tbuf[my_rows, :] = kv_two[side]
        qbuf[q_rows, :] = q_all[side]

        def gathered(i, buf):
            for l in range(levels):
                @pl.when(l == level)
                def _(l=l):
                    take(buf.at[pl.ds(0, 3 * rows)], recv_kv.at[i, l])

                @pl.when(l != level)
                def _(l=l):
                    take(buf.at[pl.ds(0, group)], recv_kv.at[i, l])

        lane = lax.broadcasted_iota(jnp.int32, (part, 2 * LANES), 1)

        def heads_at(off):
            return (
                jnp.logical_and(lane >= off, lane < off + HD),
                jnp.logical_and(lane >= off + HD, lane < off + 2 * HD),
            )

        def attend(query, off, keys, values, value_off):
            first, second = heads_at(off)
            zero = jnp.zeros_like(query)
            query = jnp.concatenate(
                [jnp.where(first, query, zero), jnp.where(second, query, zero)], axis=0
            )
            scores = lax.dot_general(
                query, keys, (((1,), (1,)), ((), ())), preferred_element_type=jnp.float32
            )
            expd = jnp.exp2(scores * (float(HD) ** (-0.5) * LOG2E))
            total = jnp.sum(expd, axis=-1, keepdims=True)
            weighted = jnp.dot(
                expd.astype(jnp.bfloat16), values, preferred_element_type=jnp.float32
            ) * (1.0 / total)
            first, second = heads_at(value_off)
            return jnp.where(first, weighted[:part], jnp.where(second, weighted[part:], 0.0))

        def send_back(src, dst, send, recv):
            for i in range(part // rows):
                b, c = half * (blks // 2) + i // 2, i % 2
                home = jnp.logical_and(b == blk, uly == c)

                @pl.when(jnp.logical_not(home))
                def _(i=i, b=b, c=c):
                    pltpu.make_async_remote_copy(
                        src_ref=src.at[pl.ds(i * rows, rows)],
                        dst_ref=dst.at[side],
                        send_sem=send,
                        recv_sem=recv.at[side],
                        device_id={"blk": b, "uly": c},
                        device_id_type=MESH,
                    ).start()

            dst[side] = src[q_rows, :]

        take(qbuf.at[pl.ds(0, part - rows)], recv_q)
        gathered(0, vbuf)
        gathered(1, kbuf)
        low = attend(qbuf[:, 0:2 * LANES], 0, kbuf[:, 0:2 * LANES], vbuf[:, 0:2 * LANES], 0)
        high = attend(
            qbuf[:, LANES:wide], pair - LANES, kbuf[:, LANES:wide], vbuf[:, LANES:wide], pair - LANES
        )
        four[...] = jnp.concatenate(
            [low[:, :LANES], low[:, LANES:] + high[:, :LANES], high[:, LANES:]], axis=1
        ).astype(jnp.bfloat16)
        send_back(four, back4, send4, recv4)
        gathered(2, tbuf)
        two[...] = attend(
            qbuf[:, wide:], 0, tbuf[:, 0:2 * LANES], tbuf[:, LANES:], pair - LANES
        ).astype(jnp.bfloat16)
        send_back(two, back2, send2, recv2)

    load_w.wait()
    give_w.wait_recv()

    def project(back, recv, s, start, own):
        if own:
            pl.when(jnp.logical_not(is_owner))(lambda: take(back.at[0], recv.at[s]))
        else:
            take(back.at[0], recv.at[s])
        return jnp.dot(
            back[s],
            w_vmem[pl.ds(pl.multiple_of(start, LANES // 2), back.shape[2]), :],
            preferred_element_type=jnp.float32,
        )

    def project4(s, own):
        return project(back4, recv4, s, s * last, own)

    def project2(s, own):
        return project(back2, recv2, s, wide + LANES - pair + s * pair, own)

    acc[...] = project4(side, True)
    acc[...] += project4(1 - side, False)
    acc[...] += project2(side, True)
    out_ref[...] = (acc[...] + project2(1 - side, False)).astype(out_ref.dtype)

    give_w.wait_send()
    slab = tbuf.at[pl.ds(0, rows)]
    for i in range(9):
        take(slab, send_kv)
    take(qbuf.at[pl.ds(0, rows)], send_q)

    @pl.when(is_owner)
    def _():
        take(four.at[pl.ds(0, part - rows)], send4)
        take(two.at[pl.ds(0, part - rows)], send2)

    @pl.when(jnp.logical_not(is_owner))
    def _():
        for i in range(3):
            take(slab, send_kv)
        take(qbuf.at[pl.ds(0, rows)], send_q)


def on_device_gather(blks, query, key, value, q_gain, k_gain, out_weight):
    rows, width = query.shape
    heads = width // HD
    depth, cols = out_weight.shape
    levels = blks // 2
    seq = 2 * blks * rows
    wide, pair, two = 4 * HD, 2 * HD, 2 * LANES
    dma = pltpu.SemaphoreType.DMA
    bf16 = jnp.bfloat16
    return pl.pallas_call(
        functools.partial(gather_kernel, blks, heads),
        out_shape=pltpu.VMEM((rows, cols), bf16),
        in_specs=[pl.BlockSpec(memory_space=pltpu.HBM)] * 6,
        out_specs=pl.BlockSpec(memory_space=pltpu.VMEM),
        scratch_shapes=[
            pltpu.VMEM((3, rows, width), bf16),
            pltpu.VMEM((2, 1, HD), jnp.float32),
            pltpu.VMEM((2, rows, wide), bf16),
            pltpu.VMEM((2, rows, 2 * pair), bf16),
            pltpu.VMEM((2, rows, wide + two), bf16),
            pltpu.VMEM((seq, wide), bf16),
            pltpu.VMEM((seq, wide), bf16),
            pltpu.VMEM((seq, 2 * pair), bf16),
            pltpu.VMEM((seq // 2, wide + two), bf16),
            pltpu.VMEM((seq // 2, wide), bf16),
            pltpu.VMEM((seq // 2, two), bf16),
            pltpu.VMEM((2, rows, wide), bf16),
            pltpu.VMEM((2, rows, two), bf16),
            pltpu.VMEM((rows, cols), jnp.float32),
            pltpu.VMEM((width, cols), bf16),
            dma((3,)),
            dma, dma, dma, dma, dma, dma, dma,
            dma((3, levels)),
            dma,
            dma((2,)),
            dma((2,)),
            dma,
            pltpu.SemaphoreType.REGULAR((2,)),
        ],
        compiler_params=pltpu.CompilerParams(collective_id=0, has_side_effects=True),
    )(query, key, value, q_gain.reshape(1, HD), k_gain.reshape(1, HD), out_weight)


def fits_gather(blks, ulys, width):
    heads = width // HD
    return ulys == 2 and blks % 4 == 0 and blks <= heads and heads // 2 == 6 and width % LANES == 0


def solution(mesh):
    blks, ulys = mesh.shape["blk"], mesh.shape["uly"]
    tokens = P(("grp", "blk", "uly"), None)

    def body(query, *rest):
        if fits_gather(blks, ulys, query.shape[1]):
            return on_device_gather(blks, query, *rest)
        return on_device(blks, ulys, query, *rest)

    return jax.shard_map(
        body,
        mesh=mesh,
        in_specs=(tokens, tokens, tokens, P(), P(), P("uly", None)),
        out_specs=tokens,
        check_vma=False,
    )
```

```python
import functools

import jax
import jax.numpy as jnp
from jax import lax
from jax.experimental import pallas as pl
from jax.experimental.pallas import tpu as pltpu
from jax.sharding import PartitionSpec as P

HD = 96
LANES = 128
CHUNKS = 1
GROUPS = 4
LOG2E = 1.4426950408889634
MESH = pl.DeviceIdType.MESH


def loop(count, body):
    if count <= 32:
        for i in range(count):
            body(i)
    else:
        lax.fori_loop(0, count, lambda i, c: (body(i), c)[1], 0)


def take(ref, sem):
    pltpu.make_async_copy(ref, ref, sem).wait()


def layer_kernel(
    blks, ulys, heads, copies,
    q_hbm, k_hbm, v_hbm, qg_hbm, kg_hbm, w_hbm, out_ref,
    raw, gains, w_vmem, pack, qkv, attn, back, acc,
    load_sem, gain_sem, w_sem, send1, recv1, send2, recv2, send_w, recv_w,
):
    n = blks * ulys
    rows = raw.shape[1]
    owners = heads * copies
    blk, uly = lax.axis_index("blk"), lax.axis_index("uly")
    me = blk * ulys + uly
    seq = n * rows
    block = seq // copies
    chunks = CHUNKS
    chunk = block // chunks
    groups = recv2.shape[0]
    members = heads // groups
    targets = chunk // rows
    depth = w_hbm.shape[0]
    upper = (2 * me) // n

    barrier = pltpu.get_barrier_semaphore()

    def greet(i):
        d = lax.rem(me + n // 2 + i + i // (n // 2), n)
        pl.semaphore_signal(
            barrier, inc=1, device_id={"blk": d // ulys, "uly": d % ulys}, device_id_type=MESH
        )

    loop(n - 1, greet)

    loads = [
        pltpu.make_async_copy(src, raw.at[i], load_sem.at[i])
        for i, src in enumerate((q_hbm, k_hbm, v_hbm))
    ]
    load_gains = [
        pltpu.make_async_copy(src, gains.at[i], gain_sem)
        for i, src in enumerate((qg_hbm, kg_hbm))
    ]
    for one in loads + load_gains:
        one.start()

    def mirror(d):
        plane = d // 4
        return d + (plane % 2) * (3 - 2 * (d % 4))

    def owner_device(o):
        return mirror(o * n // owners)

    spot = mirror(me)
    slot = (spot * owners + n - 1) // n
    is_owner = jnp.logical_and(slot < owners, (slot * n) // owners == spot)
    slot = jnp.minimum(slot, owners - 1)

    my_depth = pl.ds(pl.multiple_of(uly * depth, depth), depth)
    load_w = pltpu.make_async_copy(w_hbm, w_vmem.at[my_depth], w_sem)
    load_w.start()

    pad = jnp.zeros((rows, LANES - HD), jnp.bfloat16)
    take(gains, gain_sem)
    for i in range(2):
        loads[i].wait()
        gain = gains[i]
        for h in range(heads):
            x = raw[i, :, h * HD:(h + 1) * HD].astype(jnp.float32)
            scale = lax.rsqrt(jnp.mean(x * x, axis=-1, keepdims=True) + 1e-06)
            normed = (x * scale * gain).astype(jnp.bfloat16)
            pack[h, :, i * LANES:(i + 1) * LANES] = jnp.concatenate([normed, pad], axis=1)
    loads[2].wait()
    for h in range(heads):
        x = raw[2, :, h * HD:(h + 1) * HD]
        pack[h, :, 2 * LANES:3 * LANES] = jnp.concatenate([x, pad], axis=1)

    pl.semaphore_wait(barrier, n - 1)

    my_rows = pl.ds(pl.multiple_of(me * rows, rows), rows)

    def send_of(o):
        d = owner_device(o)
        return d, pltpu.make_async_remote_copy(
            src_ref=pack.at[o // copies],
            dst_ref=qkv.at[my_rows],
            send_sem=send1,
            recv_sem=recv1,
            device_id={"blk": d // ulys, "uly": d % ulys},
            device_id_type=MESH,
        )

    def send(i):
        d, copy = send_of(owners - 1 - i + upper * (2 * i + 1 - owners))

        @pl.when(d != me)
        def _():
            copy.start()

    loop(owners, send)

    give_w = pltpu.make_async_remote_copy(
        src_ref=w_hbm,
        dst_ref=w_vmem.at[my_depth],
        send_sem=send_w,
        recv_sem=recv_w,
        device_id={"blk": blk, "uly": 1 - uly},
        device_id_type=MESH,
    )
    give_w.start()

    @pl.when(is_owner)
    def _():
        head = slot // copies
        part = slot % copies
        qkv[my_rows, :] = pack[head]

        take(qkv.at[pl.ds(0, (n - 1) * rows)], recv1)
        score_scale = float(HD) ** (-0.5)

        def step(query, j, carry):
            weighted, total = carry
            here = pl.ds(j * block, block)
            keys = qkv[here, LANES:2 * LANES]
            values = qkv[here, 2 * LANES:3 * LANES]
            scores = lax.dot_general(
                query, keys, (((1,), (1,)), ((), ())), preferred_element_type=jnp.float32
            ) * score_scale
            expd = jnp.exp(scores)
            total = total + jnp.sum(expd, axis=-1, keepdims=True)
            weighted = weighted + jnp.dot(
                expd.astype(jnp.bfloat16), values, preferred_element_type=jnp.float32
            )
            return weighted, total

        def result_copies(c):
            for k in range(targets):
                i = targets - 1 - k + upper * (2 * k + 1 - targets)
                d = (part * chunks + c) * targets + i
                src = attn.at[pl.ds(pl.multiple_of((c * targets + i) * rows, rows), rows)]
                yield (
                    d == me,
                    functools.partial(
                        pltpu.make_async_copy, src, back.at[head], recv2.at[head // members]
                    ),
                    pltpu.make_async_remote_copy(
                        src_ref=src,
                        dst_ref=back.at[head],
                        send_sem=send2,
                        recv_sem=recv2.at[head // members],
                        device_id={"blk": d // ulys, "uly": d % ulys},
                        device_id_type=MESH,
                    ),
                )

        for k in range(chunks):
            c = chunks - 1 - k + upper * (2 * k + 1 - chunks)
            at = part * block + c * chunk
            query = qkv[pl.ds(pl.multiple_of(at, chunk), chunk), 0:LANES]
            carry = (jnp.zeros((chunk, LANES), jnp.float32), jnp.zeros((chunk, 1), jnp.float32))
            if copies == 1:
                weighted, total = step(query, 0, carry)
            else:
                weighted, total = lax.fori_loop(
                    0, copies, functools.partial(lambda q, j, c: step(q, j, c), query), carry
                )
            attn[pl.ds(pl.multiple_of(c * chunk, chunk), chunk), :] = (weighted / total).astype(jnp.bfloat16)
            for home, local, remote in result_copies(c):
                pl.when(home)(lambda local=local: local().start())
                pl.when(jnp.logical_not(home))(remote.start)

    load_w.wait()
    give_w.wait_recv()
    first = (me * groups) // n
    for i in range(groups):
        g = lax.rem(first + i * (1 - 2 * upper) + groups, groups)
        take(back.at[pl.ds(g * members, members)], recv2.at[g])
        for j in range(members):
            h = g * members + j
            term = jnp.dot(
                back[h, :, 0:HD],
                w_vmem[pl.ds(pl.multiple_of(h * HD, HD), HD), :],
                preferred_element_type=jnp.float32,
            )
            if i == 0 and j == 0:
                acc[...] = term
            elif i < groups - 1 or j < members - 1:
                acc[...] += term
            else:
                out_ref[...] = (acc[...] + term).astype(out_ref.dtype)

    give_w.wait_send()
    for i in range(copies - 1):
        take(pack, send1)

    @pl.when(is_owner)
    def _():
        take(pack.at[pl.ds(0, heads - 1)], send1)
        at_home = (slot % copies) * block == (me * rows) // block * block
        pl.when(at_home)(lambda: take(attn.at[pl.ds(0, block - rows)], send2))
        pl.when(jnp.logical_not(at_home))(lambda: take(attn, send2))

    @pl.when(jnp.logical_not(is_owner))
    def _():
        take(pack, send1)


def on_device(blks, ulys, query, key, value, q_gain, k_gain, out_weight):
    rows, width = query.shape
    heads = width // HD
    n = blks * ulys
    copies = 1
    while heads * copies * 2 <= n:
        copies *= 2
    owners = heads * copies
    depth, cols = out_weight.shape
    seq = n * rows
    block = seq // copies
    dma = pltpu.SemaphoreType.DMA
    return pl.pallas_call(
        functools.partial(layer_kernel, blks, ulys, heads, copies),
        out_shape=pltpu.VMEM((rows, cols), jnp.bfloat16),
        in_specs=[pl.BlockSpec(memory_space=pltpu.HBM)] * 6,
        out_specs=pl.BlockSpec(memory_space=pltpu.VMEM),
        scratch_shapes=[
            pltpu.VMEM((3, rows, width), jnp.bfloat16),
            pltpu.VMEM((2, 1, HD), jnp.float32),
            pltpu.VMEM((width, cols), jnp.bfloat16),
            pltpu.VMEM((heads, rows, 3 * LANES), jnp.bfloat16),
            pltpu.VMEM((seq, 3 * LANES), jnp.bfloat16),
            pltpu.VMEM((block, LANES), jnp.bfloat16),
            pltpu.VMEM((heads, rows, LANES), jnp.bfloat16),
            pltpu.VMEM((rows, cols), jnp.float32),
            dma((3,)),
            dma,
            dma,
            dma,
            dma,
            dma,
            dma((GROUPS,)),
            dma,
            dma,
        ],
        compiler_params=pltpu.CompilerParams(collective_id=0, has_side_effects=True),
    )(query, key, value, q_gain.reshape(1, HD), k_gain.reshape(1, HD), out_weight)


def gather_kernel(
    blks, heads,
    q_hbm, k_hbm, v_hbm, qg_hbm, kg_hbm, w_hbm, out_ref,
    raw, gains, k_four, kv_two, q_all, kbuf, vbuf, tbuf, qbuf, four, two, back4, back2, acc, w_vmem,
    load_sem, gain_sem, w_sem, send_kv, send_q, send4, send2, send_w,
    recv_kv, recv_q, recv4, recv2, recv_w, ready,
):
    levels = blks // 2
    rows, width = raw.shape[1:]
    wide, pair = 4 * HD, 2 * HD
    last = width - wide
    group = 4 * rows
    half_levels = levels // 2
    part = half_levels * group
    blk, uly = lax.axis_index("blk"), lax.axis_index("uly")
    level, side = blk // 2, blk % 2
    me = blk * 2 + uly
    half = level // half_levels
    owners = [(h, s, (half_levels - 1 + h) * 2 + s) for h in range(2) for s in range(2)]
    is_owner = functools.reduce(
        jnp.logical_or, [jnp.logical_and(uly == 1, blk == b) for _, _, b in owners]
    )
    my_rows = pl.ds(pl.multiple_of(me * rows, rows), rows)
    depth = w_hbm.shape[0]
    my_depth = pl.ds(pl.multiple_of(uly * depth, depth), depth)

    load_gains = [
        pltpu.make_async_copy(src, gains.at[i], gain_sem)
        for i, src in enumerate((qg_hbm, kg_hbm))
    ]
    loads = [
        pltpu.make_async_copy(src, raw.at[i], load_sem.at[i])
        for i, src in enumerate((q_hbm, k_hbm, v_hbm))
    ]
    for one in (loads[2], loads[1], *load_gains, loads[0]):
        one.start()

    barrier = pltpu.get_barrier_semaphore()
    late = half == 1
    for d in range(2 * blks):
        b, c = d // 2, d % 2
        cond = jnp.logical_or(
            jnp.logical_and(blk == b, uly == 1 - c),
            jnp.logical_and(is_owner, me != d if b >= blks // 2 else jnp.logical_and(me != d, jnp.logical_not(late))),
        )
        if c == 1 and b in [o[2] for o in owners[2:]]:
            cond = jnp.logical_or(cond, jnp.logical_not(late))

        @pl.when(cond)
        def _(b=b, c=c):
            pl.semaphore_signal(
                barrier, inc=1, device_id={"blk": b, "uly": c}, device_id_type=MESH
            )

    load_w = pltpu.make_async_copy(w_hbm, w_vmem.at[my_depth], w_sem)
    load_w.start()

    owner_here = functools.reduce(jnp.logical_or, [blk == b for _, _, b in owners])
    heard = 3 + 2 * half - owner_here.astype(jnp.int32)
    heard += jnp.where(jnp.logical_and(is_owner, late), blks - 2, 0)
    pl.semaphore_wait(barrier, heard)

    @pl.when(jnp.logical_and(is_owner, late))
    def _():
        for d in range(blks):
            pl.semaphore_signal(
                ready.at[side], inc=1, device_id={"blk": d // 2, "uly": d % 2}, device_id_type=MESH
            )

    def give(src, dst, owner, send, recv):
        h, s = owner
        return pltpu.make_async_remote_copy(
            src_ref=src,
            dst_ref=dst,
            send_sem=send,
            recv_sem=recv,
            device_id={"blk": (half_levels - 1 + h) * 2 + s, "uly": 1},
            device_id_type=MESH,
        )

    def v_four(s):
        return raw.at[2, :, pl.ds(pl.multiple_of(s * last, LANES), wide)]

    def give_v(owner):
        return give(v_four(owner[1]), vbuf.at[my_rows], owner, send_kv, recv_kv.at[0])

    def give_k(owner):
        return give(k_four.at[owner[1]], kbuf.at[my_rows], owner, send_kv, recv_kv.at[1])

    def give_two(owner):
        return give(kv_two.at[owner[1]], tbuf.at[my_rows], owner, send_kv, recv_kv.at[2])

    mine = me - half * blks
    q_rows = pl.ds(pl.multiple_of(mine * rows, rows), rows)

    def give_q(owner):
        return give(q_all.at[owner[1]], qbuf.at[q_rows], owner, send_q, recv_q)

    def across(h, *gives):
        for one in gives:
            one((h, 1 - side)).start()

    def along(h, *gives):
        here = jnp.logical_and(uly == 1, blk == (half_levels - 1 + h) * 2 + side)

        @pl.when(jnp.logical_not(here))
        def _():
            for one in gives:
                one((h, side)).start()

    def normalize(i, g):
        tiled = jnp.concatenate([gains[i]] * 4, axis=1)
        lane = lax.broadcasted_iota(jnp.int32, (rows, LANES), 1)
        tiles = [
            raw[i, :, (3 * g + t) * LANES:(3 * g + t + 1) * LANES].astype(jnp.float32)
            for t in range(3)
        ]
        squares = [t * t for t in tiles]

        def share(t, h):
            low, high = h * HD - t * LANES, (h + 1) * HD - t * LANES
            return jnp.logical_and(lane >= low, lane < high)

        scales = []
        for h in range(4):
            parts = [
                jnp.where(share(t, h), squares[t], 0.0)
                for t in range(3)
                if h * HD < (t + 1) * LANES and (h + 1) * HD > t * LANES
            ]
            total = jnp.sum(functools.reduce(jnp.add, parts), axis=-1, keepdims=True)
            scales.append(lax.rsqrt(total * (1.0 / HD) + 1e-06))
        return jnp.concatenate(
            [
                tiles[t]
                * jnp.where(share(t, t), scales[t], scales[t + 1])
                * tiled[:, t * LANES:(t + 1) * LANES]
                for t in range(3)
            ],
            axis=1,
        ).astype(jnp.bfloat16)

    loads[2].wait()
    across(0, give_v)
    take(gains, gain_sem)
    loads[1].wait()
    for s in range(2):
        k_four[s] = normalize(1, 2 * s)
    across(0, give_k)
    along(0, give_v, give_k)
    middle = normalize(1, 1)
    for s in range(2):
        kv_two[s] = jnp.concatenate(
            [middle[:, s * pair:(s + 1) * pair], raw[2, :, wide + s * pair:wide + (s + 1) * pair]],
            axis=1,
        )
    across(0, give_two)
    along(0, give_two)
    loads[0].wait()
    middle = normalize(0, 1)
    pad = jnp.zeros((rows, 2 * LANES - pair), jnp.bfloat16)
    for s in range(2):
        q_all[s, :, 0:wide] = normalize(0, 2 * s)
        q_all[s, :, wide:] = jnp.concatenate([middle[:, s * pair:(s + 1) * pair], pad], axis=1)

    @pl.when(half == 0)
    def _():
        across(0, give_q)
        along(0, give_q)

    @pl.when(jnp.logical_not(late))
    def _():
        for i in range(2):
            pl.semaphore_wait(ready.at[i], 1)

    across(1, give_v, give_k, give_two)
    along(1, give_v, give_k, give_two)

    @pl.when(half == 1)
    def _():
        across(1, give_q)
        along(1, give_q)

    give_w = pltpu.make_async_remote_copy(
        src_ref=w_hbm,
        dst_ref=w_vmem.at[my_depth],
        send_sem=send_w,
        recv_sem=recv_w,
        device_id={"uly": 1 - uly},
        device_id_type=MESH,
    )

    give_w.start()

    @pl.when(is_owner)
    def _():
        kbuf[my_rows, :] = k_four[side]
        vbuf[my_rows, :] = v_four(side)[...]
        tbuf[my_rows, :] = kv_two[side]
        qbuf[q_rows, :] = q_all[side]

        def gathered(i, buf):
            take(buf.at[pl.ds(0, buf.shape[0] - rows)], recv_kv.at[i])

        lane = lax.broadcasted_iota(jnp.int32, (part, 2 * LANES), 1)

        def heads_at(off):
            return (
                jnp.logical_and(lane >= off, lane < off + HD),
                jnp.logical_and(lane >= off + HD, lane < off + 2 * HD),
            )

        def attend(query, off, keys, values, value_off):
            first, second = heads_at(off)
            zero = jnp.zeros_like(query)
            query = jnp.concatenate(
                [jnp.where(first, query, zero), jnp.where(second, query, zero)], axis=0
            )
            scores = lax.dot_general(
                query, keys, (((1,), (1,)), ((), ())), preferred_element_type=jnp.float32
            )
            expd = jnp.exp2(scores * (float(HD) ** (-0.5) * LOG2E))
            total = jnp.sum(expd, axis=-1, keepdims=True)
            weighted = jnp.dot(
                expd.astype(jnp.bfloat16), values, preferred_element_type=jnp.float32
            ) * (1.0 / total)
            first, second = heads_at(value_off)
            return jnp.where(first, weighted[:part], jnp.where(second, weighted[part:], 0.0))

        def send_back(src, dst, send, recv):
            for k in range(part // rows - 1):
                i = k + (k >= mine).astype(jnp.int32)
                pltpu.make_async_remote_copy(
                    src_ref=src.at[pl.ds(pl.multiple_of(i * rows, rows), rows)],
                    dst_ref=dst.at[side],
                    send_sem=send,
                    recv_sem=recv.at[side],
                    device_id={"blk": half * (blks // 2) + i // 2, "uly": i % 2},
                    device_id_type=MESH,
                ).start()

            dst[side] = src[q_rows, :]

        take(qbuf.at[pl.ds(0, part - rows)], recv_q)
        gathered(0, vbuf)
        gathered(1, kbuf)
        low = attend(qbuf[:, 0:2 * LANES], 0, kbuf[:, 0:2 * LANES], vbuf[:, 0:2 * LANES], 0)
        high = attend(
            qbuf[:, LANES:wide], pair - LANES, kbuf[:, LANES:wide], vbuf[:, LANES:wide], pair - LANES
        )
        four[...] = jnp.concatenate(
            [low[:, :LANES], low[:, LANES:] + high[:, :LANES], high[:, LANES:]], axis=1
        ).astype(jnp.bfloat16)
        send_back(four, back4, send4, recv4)
        gathered(2, tbuf)
        two[...] = attend(
            qbuf[:, wide:], 0, tbuf[:, 0:2 * LANES], tbuf[:, LANES:], pair - LANES
        ).astype(jnp.bfloat16)
        send_back(two, back2, send2, recv2)

    load_w.wait()
    give_w.wait_recv()

    def project(back, recv, s, start, own):
        if own:
            pl.when(jnp.logical_not(is_owner))(lambda: take(back.at[0], recv.at[s]))
        else:
            take(back.at[0], recv.at[s])
        return jnp.dot(
            back[s],
            w_vmem[pl.ds(pl.multiple_of(start, LANES // 2), back.shape[2]), :],
            preferred_element_type=jnp.float32,
        )

    def project4(s, own):
        return project(back4, recv4, s, s * last, own)

    def project2(s, own):
        return project(back2, recv2, s, wide + LANES - pair + s * pair, own)

    acc[...] = project4(side, True)
    acc[...] += project4(1 - side, False)
    acc[...] += project2(side, True)
    out_ref[...] = (acc[...] + project2(1 - side, False)).astype(out_ref.dtype)

    give_w.wait_send()
    slab = tbuf.at[pl.ds(0, rows)]
    for i in range(9):
        take(slab, send_kv)
    take(qbuf.at[pl.ds(0, rows)], send_q)

    @pl.when(is_owner)
    def _():
        take(four.at[pl.ds(0, part - rows)], send4)
        take(two.at[pl.ds(0, part - rows)], send2)

    @pl.when(jnp.logical_not(is_owner))
    def _():
        for i in range(3):
            take(slab, send_kv)
        take(qbuf.at[pl.ds(0, rows)], send_q)


def on_device_gather(blks, query, key, value, q_gain, k_gain, out_weight):
    rows, width = query.shape
    heads = width // HD
    depth, cols = out_weight.shape
    levels = blks // 2
    seq = 2 * blks * rows
    wide, pair, two = 4 * HD, 2 * HD, 2 * LANES
    dma = pltpu.SemaphoreType.DMA
    bf16 = jnp.bfloat16
    return pl.pallas_call(
        functools.partial(gather_kernel, blks, heads),
        out_shape=pltpu.VMEM((rows, cols), bf16),
        in_specs=[pl.BlockSpec(memory_space=pltpu.HBM)] * 6,
        out_specs=pl.BlockSpec(memory_space=pltpu.VMEM),
        scratch_shapes=[
            pltpu.VMEM((3, rows, width), bf16),
            pltpu.VMEM((2, 1, HD), jnp.float32),
            pltpu.VMEM((2, rows, wide), bf16),
            pltpu.VMEM((2, rows, 2 * pair), bf16),
            pltpu.VMEM((2, rows, wide + two), bf16),
            pltpu.VMEM((seq, wide), bf16),
            pltpu.VMEM((seq, wide), bf16),
            pltpu.VMEM((seq, 2 * pair), bf16),
            pltpu.VMEM((seq // 2, wide + two), bf16),
            pltpu.VMEM((seq // 2, wide), bf16),
            pltpu.VMEM((seq // 2, two), bf16),
            pltpu.VMEM((2, rows, wide), bf16),
            pltpu.VMEM((2, rows, two), bf16),
            pltpu.VMEM((rows, cols), jnp.float32),
            pltpu.VMEM((width, cols), bf16),
            dma((3,)),
            dma, dma, dma, dma, dma, dma, dma,
            dma((3,)),
            dma,
            dma((2,)),
            dma((2,)),
            dma,
            pltpu.SemaphoreType.REGULAR((2,)),
        ],
        compiler_params=pltpu.CompilerParams(collective_id=0, has_side_effects=True),
    )(query, key, value, q_gain.reshape(1, HD), k_gain.reshape(1, HD), out_weight)


def fits_gather(blks, ulys, width):
    heads = width // HD
    return ulys == 2 and blks % 4 == 0 and blks <= heads and heads // 2 == 6 and width % LANES == 0


def solution(mesh):
    blks, ulys = mesh.shape["blk"], mesh.shape["uly"]
    tokens = P(("grp", "blk", "uly"), None)

    def body(query, *rest):
        if fits_gather(blks, ulys, query.shape[1]):
            return on_device_gather(blks, query, *rest)
        return on_device(blks, ulys, query, *rest)

    return jax.shard_map(
        body,
        mesh=mesh,
        in_specs=(tokens, tokens, tokens, P(), P(), P("uly", None)),
        out_specs=tokens,
        check_vma=False,
    )
```

```python
import functools

import jax
import jax.numpy as jnp
from jax import lax
from jax.experimental import pallas as pl
from jax.experimental.pallas import tpu as pltpu
from jax.sharding import PartitionSpec as P

HD = 96
LANES = 128
CHUNKS = 1
GROUPS = 4
LOG2E = 1.4426950408889634
MESH = pl.DeviceIdType.MESH


def loop(count, body):
    if count <= 32:
        for i in range(count):
            body(i)
    else:
        lax.fori_loop(0, count, lambda i, c: (body(i), c)[1], 0)


def take(ref, sem):
    pltpu.make_async_copy(ref, ref, sem).wait()


def layer_kernel(
    blks, ulys, heads, copies,
    q_hbm, k_hbm, v_hbm, qg_hbm, kg_hbm, w_hbm, out_ref,
    raw, gains, w_vmem, pack, qkv, attn, back, acc,
    load_sem, gain_sem, w_sem, send1, recv1, send2, recv2, send_w, recv_w,
):
    n = blks * ulys
    rows = raw.shape[1]
    owners = heads * copies
    blk, uly = lax.axis_index("blk"), lax.axis_index("uly")
    me = blk * ulys + uly
    seq = n * rows
    block = seq // copies
    chunks = CHUNKS
    chunk = block // chunks
    groups = recv2.shape[0]
    members = heads // groups
    targets = chunk // rows
    depth = w_hbm.shape[0]
    upper = (2 * me) // n

    barrier = pltpu.get_barrier_semaphore()

    def greet(i):
        d = lax.rem(me + n // 2 + i + i // (n // 2), n)
        pl.semaphore_signal(
            barrier, inc=1, device_id={"blk": d // ulys, "uly": d % ulys}, device_id_type=MESH
        )

    loop(n - 1, greet)

    loads = [
        pltpu.make_async_copy(src, raw.at[i], load_sem.at[i])
        for i, src in enumerate((q_hbm, k_hbm, v_hbm))
    ]
    load_gains = [
        pltpu.make_async_copy(src, gains.at[i], gain_sem)
        for i, src in enumerate((qg_hbm, kg_hbm))
    ]
    for one in loads + load_gains:
        one.start()

    def mirror(d):
        plane = d // 4
        return d + (plane % 2) * (3 - 2 * (d % 4))

    def owner_device(o):
        return mirror(o * n // owners)

    spot = mirror(me)
    slot = (spot * owners + n - 1) // n
    is_owner = jnp.logical_and(slot < owners, (slot * n) // owners == spot)
    slot = jnp.minimum(slot, owners - 1)

    my_depth = pl.ds(pl.multiple_of(uly * depth, depth), depth)
    load_w = pltpu.make_async_copy(w_hbm, w_vmem.at[my_depth], w_sem)
    load_w.start()

    pad = jnp.zeros((rows, LANES - HD), jnp.bfloat16)
    take(gains, gain_sem)
    for i in range(2):
        loads[i].wait()
        gain = gains[i]
        for h in range(heads):
            x = raw[i, :, h * HD:(h + 1) * HD].astype(jnp.float32)
            scale = lax.rsqrt(jnp.mean(x * x, axis=-1, keepdims=True) + 1e-06)
            normed = (x * scale * gain).astype(jnp.bfloat16)
            pack[h, :, i * LANES:(i + 1) * LANES] = jnp.concatenate([normed, pad], axis=1)
    loads[2].wait()
    for h in range(heads):
        x = raw[2, :, h * HD:(h + 1) * HD]
        pack[h, :, 2 * LANES:3 * LANES] = jnp.concatenate([x, pad], axis=1)

    pl.semaphore_wait(barrier, n - 1)

    my_rows = pl.ds(pl.multiple_of(me * rows, rows), rows)

    def send_of(o):
        d = owner_device(o)
        return d, pltpu.make_async_remote_copy(
            src_ref=pack.at[o // copies],
            dst_ref=qkv.at[my_rows],
            send_sem=send1,
            recv_sem=recv1,
            device_id={"blk": d // ulys, "uly": d % ulys},
            device_id_type=MESH,
        )

    def send(i):
        d, copy = send_of(owners - 1 - i + upper * (2 * i + 1 - owners))

        @pl.when(d != me)
        def _():
            copy.start()

    loop(owners, send)

    give_w = pltpu.make_async_remote_copy(
        src_ref=w_hbm,
        dst_ref=w_vmem.at[my_depth],
        send_sem=send_w,
        recv_sem=recv_w,
        device_id={"blk": blk, "uly": 1 - uly},
        device_id_type=MESH,
    )
    give_w.start()

    @pl.when(is_owner)
    def _():
        head = slot // copies
        part = slot % copies
        qkv[my_rows, :] = pack[head]

        take(qkv.at[pl.ds(0, (n - 1) * rows)], recv1)
        score_scale = float(HD) ** (-0.5)

        def step(query, j, carry):
            weighted, total = carry
            here = pl.ds(j * block, block)
            keys = qkv[here, LANES:2 * LANES]
            values = qkv[here, 2 * LANES:3 * LANES]
            scores = lax.dot_general(
                query, keys, (((1,), (1,)), ((), ())), preferred_element_type=jnp.float32
            ) * score_scale
            expd = jnp.exp(scores)
            total = total + jnp.sum(expd, axis=-1, keepdims=True)
            weighted = weighted + jnp.dot(
                expd.astype(jnp.bfloat16), values, preferred_element_type=jnp.float32
            )
            return weighted, total

        def result_copies(c):
            for k in range(targets):
                i = targets - 1 - k + upper * (2 * k + 1 - targets)
                d = (part * chunks + c) * targets + i
                src = attn.at[pl.ds(pl.multiple_of((c * targets + i) * rows, rows), rows)]
                yield (
                    d == me,
                    functools.partial(
                        pltpu.make_async_copy, src, back.at[head], recv2.at[head // members]
                    ),
                    pltpu.make_async_remote_copy(
                        src_ref=src,
                        dst_ref=back.at[head],
                        send_sem=send2,
                        recv_sem=recv2.at[head // members],
                        device_id={"blk": d // ulys, "uly": d % ulys},
                        device_id_type=MESH,
                    ),
                )

        for k in range(chunks):
            c = chunks - 1 - k + upper * (2 * k + 1 - chunks)
            at = part * block + c * chunk
            query = qkv[pl.ds(pl.multiple_of(at, chunk), chunk), 0:LANES]
            carry = (jnp.zeros((chunk, LANES), jnp.float32), jnp.zeros((chunk, 1), jnp.float32))
            if copies == 1:
                weighted, total = step(query, 0, carry)
            else:
                weighted, total = lax.fori_loop(
                    0, copies, functools.partial(lambda q, j, c: step(q, j, c), query), carry
                )
            attn[pl.ds(pl.multiple_of(c * chunk, chunk), chunk), :] = (weighted / total).astype(jnp.bfloat16)
            for home, local, remote in result_copies(c):
                pl.when(home)(lambda local=local: local().start())
                pl.when(jnp.logical_not(home))(remote.start)

    load_w.wait()
    give_w.wait_recv()
    first = (me * groups) // n
    for i in range(groups):
        g = lax.rem(first + i * (1 - 2 * upper) + groups, groups)
        take(back.at[pl.ds(g * members, members)], recv2.at[g])
        for j in range(members):
            h = g * members + j
            term = jnp.dot(
                back[h, :, 0:HD],
                w_vmem[pl.ds(pl.multiple_of(h * HD, HD), HD), :],
                preferred_element_type=jnp.float32,
            )
            if i == 0 and j == 0:
                acc[...] = term
            elif i < groups - 1 or j < members - 1:
                acc[...] += term
            else:
                out_ref[...] = (acc[...] + term).astype(out_ref.dtype)

    give_w.wait_send()
    for i in range(copies - 1):
        take(pack, send1)

    @pl.when(is_owner)
    def _():
        take(pack.at[pl.ds(0, heads - 1)], send1)
        at_home = (slot % copies) * block == (me * rows) // block * block
        pl.when(at_home)(lambda: take(attn.at[pl.ds(0, block - rows)], send2))
        pl.when(jnp.logical_not(at_home))(lambda: take(attn, send2))

    @pl.when(jnp.logical_not(is_owner))
    def _():
        take(pack, send1)


def on_device(blks, ulys, query, key, value, q_gain, k_gain, out_weight):
    rows, width = query.shape
    heads = width // HD
    n = blks * ulys
    copies = 1
    while heads * copies * 2 <= n:
        copies *= 2
    owners = heads * copies
    depth, cols = out_weight.shape
    seq = n * rows
    block = seq // copies
    dma = pltpu.SemaphoreType.DMA
    return pl.pallas_call(
        functools.partial(layer_kernel, blks, ulys, heads, copies),
        out_shape=pltpu.VMEM((rows, cols), jnp.bfloat16),
        in_specs=[pl.BlockSpec(memory_space=pltpu.HBM)] * 6,
        out_specs=pl.BlockSpec(memory_space=pltpu.VMEM),
        scratch_shapes=[
            pltpu.VMEM((3, rows, width), jnp.bfloat16),
            pltpu.VMEM((2, 1, HD), jnp.float32),
            pltpu.VMEM((width, cols), jnp.bfloat16),
            pltpu.VMEM((heads, rows, 3 * LANES), jnp.bfloat16),
            pltpu.VMEM((seq, 3 * LANES), jnp.bfloat16),
            pltpu.VMEM((block, LANES), jnp.bfloat16),
            pltpu.VMEM((heads, rows, LANES), jnp.bfloat16),
            pltpu.VMEM((rows, cols), jnp.float32),
            dma((3,)),
            dma,
            dma,
            dma,
            dma,
            dma,
            dma((GROUPS,)),
            dma,
            dma,
        ],
        compiler_params=pltpu.CompilerParams(collective_id=0, has_side_effects=True),
    )(query, key, value, q_gain.reshape(1, HD), k_gain.reshape(1, HD), out_weight)


def gather_kernel(
    blks, heads,
    q_hbm, k_hbm, v_hbm, qg_hbm, kg_hbm, w_hbm, out_ref,
    raw, gains, k_four, kv_two, q_all, kbuf, vbuf, tbuf, qbuf, four, two, back4, back2, acc, w_vmem,
    load_sem, gain_sem, w_sem, send_kv, send_q, send4, send2, send_w,
    recv_kv, recv_q, recv4, recv2, recv_w, ready,
):
    levels = blks // 2
    rows, width = raw.shape[1:]
    wide, pair = 4 * HD, 2 * HD
    last = width - wide
    group = 4 * rows
    half_levels = levels // 2
    part = half_levels * group
    blk, uly = lax.axis_index("blk"), lax.axis_index("uly")
    level, side = blk // 2, blk % 2
    me = blk * 2 + uly
    half = level // half_levels
    owners = [(h, s, (half_levels - 1 + h) * 2 + s) for h in range(2) for s in range(2)]
    is_owner = functools.reduce(
        jnp.logical_or, [jnp.logical_and(uly == 1, blk == b) for _, _, b in owners]
    )
    my_rows = pl.ds(pl.multiple_of(me * rows, rows), rows)
    depth = w_hbm.shape[0]
    my_depth = pl.ds(pl.multiple_of(uly * depth, depth), depth)

    load_gains = [
        pltpu.make_async_copy(src, gains.at[i], gain_sem)
        for i, src in enumerate((qg_hbm, kg_hbm))
    ]
    loads = [
        pltpu.make_async_copy(src, raw.at[i], load_sem.at[i])
        for i, src in enumerate((q_hbm, k_hbm, v_hbm))
    ]
    for one in (loads[2], loads[1], *load_gains, loads[0]):
        one.start()

    barrier = pltpu.get_barrier_semaphore()
    late = half == 1
    for d in range(2 * blks):
        b, c = d // 2, d % 2
        cond = jnp.logical_or(
            jnp.logical_and(blk == b, uly == 1 - c),
            jnp.logical_and(is_owner, me != d if b >= blks // 2 else jnp.logical_and(me != d, jnp.logical_not(late))),
        )
        if c == 1 and b in [o[2] for o in owners[2:]]:
            cond = jnp.logical_or(cond, jnp.logical_not(late))

        @pl.when(cond)
        def _(b=b, c=c):
            pl.semaphore_signal(
                barrier, inc=1, device_id={"blk": b, "uly": c}, device_id_type=MESH
            )

    load_w = pltpu.make_async_copy(w_hbm, w_vmem.at[my_depth], w_sem)
    load_w.start()

    owner_here = functools.reduce(jnp.logical_or, [blk == b for _, _, b in owners])
    heard = 3 + 2 * half - owner_here.astype(jnp.int32)
    heard += jnp.where(jnp.logical_and(is_owner, late), blks - 2, 0)
    pl.semaphore_wait(barrier, heard)

    @pl.when(jnp.logical_and(is_owner, late))
    def _():
        for d in range(blks):
            pl.semaphore_signal(
                ready.at[side], inc=1, device_id={"blk": d // 2, "uly": d % 2}, device_id_type=MESH
            )

    def give(src, dst, owner, send, recv):
        h, s = owner
        return pltpu.make_async_remote_copy(
            src_ref=src,
            dst_ref=dst,
            send_sem=send,
            recv_sem=recv,
            device_id={"blk": (half_levels - 1 + h) * 2 + s, "uly": 1},
            device_id_type=MESH,
        )

    def v_four(s):
        return raw.at[2, :, pl.ds(pl.multiple_of(s * last, LANES), wide)]

    def give_v(owner):
        return give(v_four(owner[1]), vbuf.at[my_rows], owner, send_kv, recv_kv.at[0])

    def give_k(owner):
        return give(k_four.at[owner[1]], kbuf.at[my_rows], owner, send_kv, recv_kv.at[1])

    def give_two(owner):
        return give(kv_two.at[owner[1]], tbuf.at[my_rows], owner, send_kv, recv_kv.at[2])

    mine = me - half * blks
    q_rows = pl.ds(pl.multiple_of(mine * rows, rows), rows)

    def give_q(owner):
        return give(q_all.at[owner[1]], qbuf.at[q_rows], owner, send_q, recv_q)

    def across(h, *gives):
        for one in gives:
            one((h, 1 - side)).start()

    def along(h, *gives):
        here = jnp.logical_and(uly == 1, blk == (half_levels - 1 + h) * 2 + side)

        @pl.when(jnp.logical_not(here))
        def _():
            for one in gives:
                one((h, side)).start()

    def normalize(i, g):
        tiled = jnp.concatenate([gains[i]] * 4, axis=1)
        lane = lax.broadcasted_iota(jnp.int32, (rows, LANES), 1)
        tiles = [
            raw[i, :, (3 * g + t) * LANES:(3 * g + t + 1) * LANES].astype(jnp.float32)
            for t in range(3)
        ]
        squares = [t * t for t in tiles]

        def share(t, h):
            low, high = h * HD - t * LANES, (h + 1) * HD - t * LANES
            return jnp.logical_and(lane >= low, lane < high)

        scales = []
        for h in range(4):
            parts = [
                jnp.where(share(t, h), squares[t], 0.0)
                for t in range(3)
                if h * HD < (t + 1) * LANES and (h + 1) * HD > t * LANES
            ]
            total = jnp.sum(functools.reduce(jnp.add, parts), axis=-1, keepdims=True)
            scales.append(lax.rsqrt(total * (1.0 / HD) + 1e-06))
        return jnp.concatenate(
            [
                tiles[t]
                * jnp.where(share(t, t), scales[t], scales[t + 1])
                * tiled[:, t * LANES:(t + 1) * LANES]
                for t in range(3)
            ],
            axis=1,
        ).astype(jnp.bfloat16)

    loads[2].wait()
    straight = jnp.logical_and(level > half_levels, side == 0)
    pl.when(straight)(lambda: along(0, give_v))
    across(0, give_v)
    take(gains, gain_sem)
    loads[1].wait()
    for s in range(2):
        k_four[s] = normalize(1, 2 * s)
    pl.when(straight)(lambda: along(0, give_k))
    across(0, give_k)
    pl.when(jnp.logical_not(straight))(lambda: along(0, give_v, give_k))
    middle = normalize(1, 1)
    for s in range(2):
        kv_two[s] = jnp.concatenate(
            [middle[:, s * pair:(s + 1) * pair], raw[2, :, wide + s * pair:wide + (s + 1) * pair]],
            axis=1,
        )
    pl.when(straight)(lambda: along(0, give_two))
    across(0, give_two)
    pl.when(jnp.logical_not(straight))(lambda: along(0, give_two))
    loads[0].wait()
    middle = normalize(0, 1)
    pad = jnp.zeros((rows, 2 * LANES - pair), jnp.bfloat16)
    for s in range(2):
        q_all[s, :, 0:wide] = normalize(0, 2 * s)
        q_all[s, :, wide:] = jnp.concatenate([middle[:, s * pair:(s + 1) * pair], pad], axis=1)

    @pl.when(half == 0)
    def _():
        across(0, give_q)
        along(0, give_q)

    @pl.when(jnp.logical_not(late))
    def _():
        for i in range(2):
            pl.semaphore_wait(ready.at[i], 1)

    across(1, give_v, give_k, give_two)
    along(1, give_v, give_k, give_two)

    @pl.when(half == 1)
    def _():
        across(1, give_q)
        along(1, give_q)

    give_w = pltpu.make_async_remote_copy(
        src_ref=w_hbm,
        dst_ref=w_vmem.at[my_depth],
        send_sem=send_w,
        recv_sem=recv_w,
        device_id={"uly": 1 - uly},
        device_id_type=MESH,
    )

    give_w.start()

    @pl.when(is_owner)
    def _():
        kbuf[my_rows, :] = k_four[side]
        vbuf[my_rows, :] = v_four(side)[...]
        tbuf[my_rows, :] = kv_two[side]
        qbuf[q_rows, :] = q_all[side]

        def gathered(i, buf):
            take(buf.at[pl.ds(0, buf.shape[0] - rows)], recv_kv.at[i])

        lane = lax.broadcasted_iota(jnp.int32, (part, 2 * LANES), 1)

        def heads_at(off):
            return (
                jnp.logical_and(lane >= off, lane < off + HD),
                jnp.logical_and(lane >= off + HD, lane < off + 2 * HD),
            )

        def attend(query, off, keys, values, value_off):
            first, second = heads_at(off)
            zero = jnp.zeros_like(query)
            query = jnp.concatenate(
                [jnp.where(first, query, zero), jnp.where(second, query, zero)], axis=0
            )
            scores = lax.dot_general(
                query, keys, (((1,), (1,)), ((), ())), preferred_element_type=jnp.float32
            )
            expd = jnp.exp2(scores * (float(HD) ** (-0.5) * LOG2E))
            total = jnp.sum(expd, axis=-1, keepdims=True)
            weighted = jnp.dot(
                expd.astype(jnp.bfloat16), values, preferred_element_type=jnp.float32
            ) * (1.0 / total)
            first, second = heads_at(value_off)
            return jnp.where(first, weighted[:part], jnp.where(second, weighted[part:], 0.0))

        def send_back(src, dst, send, recv):
            for k in range(part // rows - 1):
                i = k + (k >= mine).astype(jnp.int32)
                pltpu.make_async_remote_copy(
                    src_ref=src.at[pl.ds(pl.multiple_of(i * rows, rows), rows)],
                    dst_ref=dst.at[side],
                    send_sem=send,
                    recv_sem=recv.at[side],
                    device_id={"blk": half * (blks // 2) + i // 2, "uly": i % 2},
                    device_id_type=MESH,
                ).start()

            dst[side] = src[q_rows, :]

        take(qbuf.at[pl.ds(0, part - rows)], recv_q)
        gathered(0, vbuf)
        gathered(1, kbuf)
        low = attend(qbuf[:, 0:2 * LANES], 0, kbuf[:, 0:2 * LANES], vbuf[:, 0:2 * LANES], 0)
        high = attend(
            qbuf[:, LANES:wide], pair - LANES, kbuf[:, LANES:wide], vbuf[:, LANES:wide], pair - LANES
        )
        four[...] = jnp.concatenate(
            [low[:, :LANES], low[:, LANES:] + high[:, :LANES], high[:, LANES:]], axis=1
        ).astype(jnp.bfloat16)
        send_back(four, back4, send4, recv4)
        gathered(2, tbuf)
        two[...] = attend(
            qbuf[:, wide:], 0, tbuf[:, 0:2 * LANES], tbuf[:, LANES:], pair - LANES
        ).astype(jnp.bfloat16)
        send_back(two, back2, send2, recv2)

    load_w.wait()
    give_w.wait_recv()

    def project(back, recv, s, start, own):
        if own:
            pl.when(jnp.logical_not(is_owner))(lambda: take(back.at[0], recv.at[s]))
        else:
            take(back.at[0], recv.at[s])
        return jnp.dot(
            back[s],
            w_vmem[pl.ds(pl.multiple_of(start, LANES // 2), back.shape[2]), :],
            preferred_element_type=jnp.float32,
        )

    def project4(s, own):
        return project(back4, recv4, s, s * last, own)

    def project2(s, own):
        return project(back2, recv2, s, wide + LANES - pair + s * pair, own)

    acc[...] = project4(side, True)
    acc[...] += project4(1 - side, False)
    acc[...] += project2(side, True)

    give_w.wait_send()
    slab = tbuf.at[pl.ds(0, rows)]
    for i in range(9):
        take(slab, send_kv)
    take(qbuf.at[pl.ds(0, rows)], send_q)
    pl.when(is_owner)(lambda: take(four.at[pl.ds(0, part - rows)], send4))

    @pl.when(jnp.logical_not(is_owner))
    def _():
        for i in range(3):
            take(slab, send_kv)
        take(qbuf.at[pl.ds(0, rows)], send_q)

    out_ref[...] = (acc[...] + project2(1 - side, False)).astype(out_ref.dtype)
    pl.when(is_owner)(lambda: take(two.at[pl.ds(0, part - rows)], send2))


def on_device_gather(blks, query, key, value, q_gain, k_gain, out_weight):
    rows, width = query.shape
    heads = width // HD
    depth, cols = out_weight.shape
    levels = blks // 2
    seq = 2 * blks * rows
    wide, pair, two = 4 * HD, 2 * HD, 2 * LANES
    dma = pltpu.SemaphoreType.DMA
    bf16 = jnp.bfloat16
    return pl.pallas_call(
        functools.partial(gather_kernel, blks, heads),
        out_shape=pltpu.VMEM((rows, cols), bf16),
        in_specs=[pl.BlockSpec(memory_space=pltpu.HBM)] * 6,
        out_specs=pl.BlockSpec(memory_space=pltpu.VMEM),
        scratch_shapes=[
            pltpu.VMEM((3, rows, width), bf16),
            pltpu.VMEM((2, 1, HD), jnp.float32),
            pltpu.VMEM((2, rows, wide), bf16),
            pltpu.VMEM((2, rows, 2 * pair), bf16),
            pltpu.VMEM((2, rows, wide + two), bf16),
            pltpu.VMEM((seq, wide), bf16),
            pltpu.VMEM((seq, wide), bf16),
            pltpu.VMEM((seq, 2 * pair), bf16),
            pltpu.VMEM((seq // 2, wide + two), bf16),
            pltpu.VMEM((seq // 2, wide), bf16),
            pltpu.VMEM((seq // 2, two), bf16),
            pltpu.VMEM((2, rows, wide), bf16),
            pltpu.VMEM((2, rows, two), bf16),
            pltpu.VMEM((rows, cols), jnp.float32),
            pltpu.VMEM((width, cols), bf16),
            dma((3,)),
            dma, dma, dma, dma, dma, dma, dma,
            dma((3,)),
            dma,
            dma((2,)),
            dma((2,)),
            dma,
            pltpu.SemaphoreType.REGULAR((2,)),
        ],
        compiler_params=pltpu.CompilerParams(collective_id=0, has_side_effects=True),
    )(query, key, value, q_gain.reshape(1, HD), k_gain.reshape(1, HD), out_weight)


def fits_gather(blks, ulys, width):
    heads = width // HD
    return ulys == 2 and blks % 4 == 0 and blks <= heads and heads // 2 == 6 and width % LANES == 0


def solution(mesh):
    blks, ulys = mesh.shape["blk"], mesh.shape["uly"]
    tokens = P(("grp", "blk", "uly"), None)

    def body(query, *rest):
        if fits_gather(blks, ulys, query.shape[1]):
            return on_device_gather(blks, query, *rest)
        return on_device(blks, ulys, query, *rest)

    return jax.shard_map(
        body,
        mesh=mesh,
        in_specs=(tokens, tokens, tokens, P(), P(), P("uly", None)),
        out_specs=tokens,
        check_vma=False,
    )
```

```python
import functools

import jax
import jax.numpy as jnp
from jax import lax
from jax.experimental import pallas as pl
from jax.experimental.pallas import tpu as pltpu
from jax.sharding import PartitionSpec as P

HD = 96
LANES = 128
CHUNKS = 1
GROUPS = 4
LOG2E = 1.4426950408889634
MESH = pl.DeviceIdType.MESH


def loop(count, body):
    if count <= 32:
        for i in range(count):
            body(i)
    else:
        lax.fori_loop(0, count, lambda i, c: (body(i), c)[1], 0)


def take(ref, sem):
    pltpu.make_async_copy(ref, ref, sem).wait()


def layer_kernel(
    blks, ulys, heads, copies,
    q_hbm, k_hbm, v_hbm, qg_hbm, kg_hbm, w_hbm, out_ref,
    raw, gains, w_vmem, pack, qkv, attn, back, acc,
    load_sem, gain_sem, w_sem, send1, recv1, send2, recv2, send_w, recv_w,
):
    n = blks * ulys
    rows = raw.shape[1]
    owners = heads * copies
    blk, uly = lax.axis_index("blk"), lax.axis_index("uly")
    me = blk * ulys + uly
    seq = n * rows
    block = seq // copies
    chunks = CHUNKS
    chunk = block // chunks
    groups = recv2.shape[0]
    members = heads // groups
    targets = chunk // rows
    depth = w_hbm.shape[0]
    upper = (2 * me) // n

    barrier = pltpu.get_barrier_semaphore()

    def greet(i):
        d = lax.rem(me + n // 2 + i + i // (n // 2), n)
        pl.semaphore_signal(
            barrier, inc=1, device_id={"blk": d // ulys, "uly": d % ulys}, device_id_type=MESH
        )

    loop(n - 1, greet)

    loads = [
        pltpu.make_async_copy(src, raw.at[i], load_sem.at[i])
        for i, src in enumerate((q_hbm, k_hbm, v_hbm))
    ]
    load_gains = [
        pltpu.make_async_copy(src, gains.at[i], gain_sem)
        for i, src in enumerate((qg_hbm, kg_hbm))
    ]
    for one in loads + load_gains:
        one.start()

    def mirror(d):
        plane = d // 4
        return d + (plane % 2) * (3 - 2 * (d % 4))

    def owner_device(o):
        return mirror(o * n // owners)

    spot = mirror(me)
    slot = (spot * owners + n - 1) // n
    is_owner = jnp.logical_and(slot < owners, (slot * n) // owners == spot)
    slot = jnp.minimum(slot, owners - 1)

    my_depth = pl.ds(pl.multiple_of(uly * depth, depth), depth)
    load_w = pltpu.make_async_copy(w_hbm, w_vmem.at[my_depth], w_sem)
    load_w.start()

    pad = jnp.zeros((rows, LANES - HD), jnp.bfloat16)
    take(gains, gain_sem)
    for i in range(2):
        loads[i].wait()
        gain = gains[i]
        for h in range(heads):
            x = raw[i, :, h * HD:(h + 1) * HD].astype(jnp.float32)
            scale = lax.rsqrt(jnp.mean(x * x, axis=-1, keepdims=True) + 1e-06)
            normed = (x * scale * gain).astype(jnp.bfloat16)
            pack[h, :, i * LANES:(i + 1) * LANES] = jnp.concatenate([normed, pad], axis=1)
    loads[2].wait()
    for h in range(heads):
        x = raw[2, :, h * HD:(h + 1) * HD]
        pack[h, :, 2 * LANES:3 * LANES] = jnp.concatenate([x, pad], axis=1)

    pl.semaphore_wait(barrier, n - 1)

    my_rows = pl.ds(pl.multiple_of(me * rows, rows), rows)

    def send_of(o):
        d = owner_device(o)
        return d, pltpu.make_async_remote_copy(
            src_ref=pack.at[o // copies],
            dst_ref=qkv.at[my_rows],
            send_sem=send1,
            recv_sem=recv1,
            device_id={"blk": d // ulys, "uly": d % ulys},
            device_id_type=MESH,
        )

    def send(i):
        d, copy = send_of(owners - 1 - i + upper * (2 * i + 1 - owners))

        @pl.when(d != me)
        def _():
            copy.start()

    loop(owners, send)

    give_w = pltpu.make_async_remote_copy(
        src_ref=w_hbm,
        dst_ref=w_vmem.at[my_depth],
        send_sem=send_w,
        recv_sem=recv_w,
        device_id={"blk": blk, "uly": 1 - uly},
        device_id_type=MESH,
    )
    give_w.start()

    @pl.when(is_owner)
    def _():
        head = slot // copies
        part = slot % copies
        qkv[my_rows, :] = pack[head]

        take(qkv.at[pl.ds(0, (n - 1) * rows)], recv1)
        score_scale = float(HD) ** (-0.5)

        def step(query, j, carry):
            weighted, total = carry
            here = pl.ds(j * block, block)
            keys = qkv[here, LANES:2 * LANES]
            values = qkv[here, 2 * LANES:3 * LANES]
            scores = lax.dot_general(
                query, keys, (((1,), (1,)), ((), ())), preferred_element_type=jnp.float32
            ) * score_scale
            expd = jnp.exp(scores)
            total = total + jnp.sum(expd, axis=-1, keepdims=True)
            weighted = weighted + jnp.dot(
                expd.astype(jnp.bfloat16), values, preferred_element_type=jnp.float32
            )
            return weighted, total

        def result_copies(c):
            for k in range(targets):
                i = targets - 1 - k + upper * (2 * k + 1 - targets)
                d = (part * chunks + c) * targets + i
                src = attn.at[pl.ds(pl.multiple_of((c * targets + i) * rows, rows), rows)]
                yield (
                    d == me,
                    functools.partial(
                        pltpu.make_async_copy, src, back.at[head], recv2.at[head // members]
                    ),
                    pltpu.make_async_remote_copy(
                        src_ref=src,
                        dst_ref=back.at[head],
                        send_sem=send2,
                        recv_sem=recv2.at[head // members],
                        device_id={"blk": d // ulys, "uly": d % ulys},
                        device_id_type=MESH,
                    ),
                )

        for k in range(chunks):
            c = chunks - 1 - k + upper * (2 * k + 1 - chunks)
            at = part * block + c * chunk
            query = qkv[pl.ds(pl.multiple_of(at, chunk), chunk), 0:LANES]
            carry = (jnp.zeros((chunk, LANES), jnp.float32), jnp.zeros((chunk, 1), jnp.float32))
            if copies == 1:
                weighted, total = step(query, 0, carry)
            else:
                weighted, total = lax.fori_loop(
                    0, copies, functools.partial(lambda q, j, c: step(q, j, c), query), carry
                )
            attn[pl.ds(pl.multiple_of(c * chunk, chunk), chunk), :] = (weighted / total).astype(jnp.bfloat16)
            for home, local, remote in result_copies(c):
                pl.when(home)(lambda local=local: local().start())
                pl.when(jnp.logical_not(home))(remote.start)

    load_w.wait()
    give_w.wait_recv()
    first = (me * groups) // n
    for i in range(groups):
        g = lax.rem(first + i * (1 - 2 * upper) + groups, groups)
        take(back.at[pl.ds(g * members, members)], recv2.at[g])
        for j in range(members):
            h = g * members + j
            term = jnp.dot(
                back[h, :, 0:HD],
                w_vmem[pl.ds(pl.multiple_of(h * HD, HD), HD), :],
                preferred_element_type=jnp.float32,
            )
            if i == 0 and j == 0:
                acc[...] = term
            elif i < groups - 1 or j < members - 1:
                acc[...] += term
            else:
                out_ref[...] = (acc[...] + term).astype(out_ref.dtype)

    give_w.wait_send()
    for i in range(copies - 1):
        take(pack, send1)

    @pl.when(is_owner)
    def _():
        take(pack.at[pl.ds(0, heads - 1)], send1)
        at_home = (slot % copies) * block == (me * rows) // block * block
        pl.when(at_home)(lambda: take(attn.at[pl.ds(0, block - rows)], send2))
        pl.when(jnp.logical_not(at_home))(lambda: take(attn, send2))

    @pl.when(jnp.logical_not(is_owner))
    def _():
        take(pack, send1)


def on_device(blks, ulys, query, key, value, q_gain, k_gain, out_weight):
    rows, width = query.shape
    heads = width // HD
    n = blks * ulys
    copies = 1
    while heads * copies * 2 <= n:
        copies *= 2
    owners = heads * copies
    depth, cols = out_weight.shape
    seq = n * rows
    block = seq // copies
    dma = pltpu.SemaphoreType.DMA
    return pl.pallas_call(
        functools.partial(layer_kernel, blks, ulys, heads, copies),
        out_shape=pltpu.VMEM((rows, cols), jnp.bfloat16),
        in_specs=[pl.BlockSpec(memory_space=pltpu.HBM)] * 6,
        out_specs=pl.BlockSpec(memory_space=pltpu.VMEM),
        scratch_shapes=[
            pltpu.VMEM((3, rows, width), jnp.bfloat16),
            pltpu.VMEM((2, 1, HD), jnp.float32),
            pltpu.VMEM((width, cols), jnp.bfloat16),
            pltpu.VMEM((heads, rows, 3 * LANES), jnp.bfloat16),
            pltpu.VMEM((seq, 3 * LANES), jnp.bfloat16),
            pltpu.VMEM((block, LANES), jnp.bfloat16),
            pltpu.VMEM((heads, rows, LANES), jnp.bfloat16),
            pltpu.VMEM((rows, cols), jnp.float32),
            dma((3,)),
            dma,
            dma,
            dma,
            dma,
            dma,
            dma((GROUPS,)),
            dma,
            dma,
        ],
        compiler_params=pltpu.CompilerParams(collective_id=0, has_side_effects=True),
    )(query, key, value, q_gain.reshape(1, HD), k_gain.reshape(1, HD), out_weight)


def gather_kernel(
    blks, heads,
    q_hbm, k_hbm, v_hbm, qg_hbm, kg_hbm, w_hbm, out_ref,
    raw, gains, k_four, kv_two, q_all, kbuf, vbuf, tbuf, qbuf, four, two, back4, back2, acc, w_vmem, stacked,
    load_sem, gain_sem, w_sem, send_kv, send_q, send4, send2, send_w,
    recv_kv, recv_q, recv4, recv2, recv_w, ready,
):
    levels = blks // 2
    rows, width = raw.shape[1:]
    wide, pair = 4 * HD, 2 * HD
    last = width - wide
    group = 4 * rows
    half_levels = levels // 2
    part = half_levels * group
    blk, uly = lax.axis_index("blk"), lax.axis_index("uly")
    level, side = blk // 2, blk % 2
    me = blk * 2 + uly
    half = level // half_levels
    owners = [(h, s, (half_levels - 1 + h) * 2 + s) for h in range(2) for s in range(2)]
    is_owner = functools.reduce(
        jnp.logical_or, [jnp.logical_and(uly == 1, blk == b) for _, _, b in owners]
    )
    my_rows = pl.ds(pl.multiple_of(me * rows, rows), rows)
    depth = w_hbm.shape[0]
    my_depth = pl.ds(pl.multiple_of(uly * depth, depth), depth)

    load_gains = [
        pltpu.make_async_copy(src, gains.at[i], gain_sem)
        for i, src in enumerate((qg_hbm, kg_hbm))
    ]
    loads = [
        pltpu.make_async_copy(src, raw.at[i], load_sem.at[i])
        for i, src in enumerate((q_hbm, k_hbm, v_hbm))
    ]
    for one in (loads[2], loads[1], *load_gains, loads[0]):
        one.start()

    barrier = pltpu.get_barrier_semaphore()
    late = half == 1
    for d in range(2 * blks):
        b, c = d // 2, d % 2
        cond = jnp.logical_or(
            jnp.logical_and(blk == b, uly == 1 - c),
            jnp.logical_and(is_owner, me != d if b >= blks // 2 else jnp.logical_and(me != d, jnp.logical_not(late))),
        )
        if c == 1 and b in [o[2] for o in owners[2:]]:
            cond = jnp.logical_or(cond, jnp.logical_not(late))

        @pl.when(cond)
        def _(b=b, c=c):
            pl.semaphore_signal(
                barrier, inc=1, device_id={"blk": b, "uly": c}, device_id_type=MESH
            )

    load_w = pltpu.make_async_copy(w_hbm, w_vmem.at[my_depth], w_sem)
    load_w.start()

    owner_here = functools.reduce(jnp.logical_or, [blk == b for _, _, b in owners])
    heard = 3 + 2 * half - owner_here.astype(jnp.int32)
    heard += jnp.where(jnp.logical_and(is_owner, late), blks - 2, 0)
    pl.semaphore_wait(barrier, heard)

    @pl.when(jnp.logical_and(is_owner, late))
    def _():
        for d in range(blks):
            pl.semaphore_signal(
                ready.at[side], inc=1, device_id={"blk": d // 2, "uly": d % 2}, device_id_type=MESH
            )

    def give(src, dst, owner, send, recv):
        h, s = owner
        return pltpu.make_async_remote_copy(
            src_ref=src,
            dst_ref=dst,
            send_sem=send,
            recv_sem=recv,
            device_id={"blk": (half_levels - 1 + h) * 2 + s, "uly": 1},
            device_id_type=MESH,
        )

    def v_four(s):
        return raw.at[2, :, pl.ds(pl.multiple_of(s * last, LANES), wide)]

    def give_v(owner):
        return give(v_four(owner[1]), vbuf.at[my_rows], owner, send_kv, recv_kv.at[0])

    def give_k(owner):
        return give(k_four.at[owner[1]], kbuf.at[my_rows], owner, send_kv, recv_kv.at[1])

    def give_two(owner):
        return give(kv_two.at[owner[1]], tbuf.at[my_rows], owner, send_kv, recv_kv.at[2])

    mine = me - half * blks
    q_rows = pl.ds(pl.multiple_of(mine * rows, rows), rows)

    def give_q(owner):
        return give(q_all.at[owner[1]], qbuf.at[q_rows], owner, send_q, recv_q)

    def across(h, *gives):
        for one in gives:
            one((h, 1 - side)).start()

    def along(h, *gives):
        here = jnp.logical_and(uly == 1, blk == (half_levels - 1 + h) * 2 + side)

        @pl.when(jnp.logical_not(here))
        def _():
            for one in gives:
                one((h, side)).start()

    def normalize(i, g):
        tiled = jnp.concatenate([gains[i]] * 4, axis=1)
        lane = lax.broadcasted_iota(jnp.int32, (rows, LANES), 1)
        tiles = [
            raw[i, :, (3 * g + t) * LANES:(3 * g + t + 1) * LANES].astype(jnp.float32)
            for t in range(3)
        ]
        squares = [t * t for t in tiles]

        def share(t, h):
            low, high = h * HD - t * LANES, (h + 1) * HD - t * LANES
            return jnp.logical_and(lane >= low, lane < high)

        scales = []
        for h in range(4):
            parts = [
                jnp.where(share(t, h), squares[t], 0.0)
                for t in range(3)
                if h * HD < (t + 1) * LANES and (h + 1) * HD > t * LANES
            ]
            total = jnp.sum(functools.reduce(jnp.add, parts), axis=-1, keepdims=True)
            scales.append(lax.rsqrt(total * (1.0 / HD) + 1e-06))
        return jnp.concatenate(
            [
                tiles[t]
                * jnp.where(share(t, t), scales[t], scales[t + 1])
                * tiled[:, t * LANES:(t + 1) * LANES]
                for t in range(3)
            ],
            axis=1,
        ).astype(jnp.bfloat16)

    loads[2].wait()
    straight = jnp.logical_and(level > half_levels, side == 0)
    pl.when(straight)(lambda: along(0, give_v))
    across(0, give_v)
    take(gains, gain_sem)
    loads[1].wait()
    for s in range(2):
        k_four[s] = normalize(1, 2 * s)
    pl.when(straight)(lambda: along(0, give_k))
    across(0, give_k)
    pl.when(jnp.logical_not(straight))(lambda: along(0, give_v, give_k))
    middle = normalize(1, 1)
    for s in range(2):
        kv_two[s] = jnp.concatenate(
            [middle[:, s * pair:(s + 1) * pair], raw[2, :, wide + s * pair:wide + (s + 1) * pair]],
            axis=1,
        )
    pl.when(straight)(lambda: along(0, give_two))
    across(0, give_two)
    pl.when(jnp.logical_not(straight))(lambda: along(0, give_two))
    loads[0].wait()
    middle = normalize(0, 1)
    pad = jnp.zeros((rows, 2 * LANES - pair), jnp.bfloat16)
    for s in range(2):
        q_all[s, :, 0:wide] = normalize(0, 2 * s)
        q_all[s, :, wide:] = jnp.concatenate([middle[:, s * pair:(s + 1) * pair], pad], axis=1)

    @pl.when(half == 0)
    def _():
        across(0, give_q)
        along(0, give_q)

    @pl.when(jnp.logical_not(late))
    def _():
        for i in range(2):
            pl.semaphore_wait(ready.at[i], 1)

    across(1, give_v, give_k, give_two)
    along(1, give_v, give_k, give_two)

    @pl.when(half == 1)
    def _():
        across(1, give_q)
        along(1, give_q)

    give_w = pltpu.make_async_remote_copy(
        src_ref=w_hbm,
        dst_ref=w_vmem.at[my_depth],
        send_sem=send_w,
        recv_sem=recv_w,
        device_id={"uly": 1 - uly},
        device_id_type=MESH,
    )

    give_w.start()

    @pl.when(is_owner)
    def _():
        kbuf[my_rows, :] = k_four[side]
        vbuf[my_rows, :] = v_four(side)[...]
        tbuf[my_rows, :] = kv_two[side]
        qbuf[q_rows, :] = q_all[side]

        def gathered(i, buf):
            take(buf.at[pl.ds(0, buf.shape[0] - rows)], recv_kv.at[i])

        lane = lax.broadcasted_iota(jnp.int32, (part, 2 * LANES), 1)

        def heads_at(off):
            return (
                jnp.logical_and(lane >= off, lane < off + HD),
                jnp.logical_and(lane >= off + HD, lane < off + 2 * HD),
            )

        def stack(j, query, off):
            first, second = heads_at(off)
            zero = jnp.zeros_like(query)
            stacked[j] = jnp.concatenate(
                [jnp.where(first, query, zero), jnp.where(second, query, zero)], axis=0
            )

        def attend(j, keys, values, value_off):
            scores = lax.dot_general(
                stacked[j], keys, (((1,), (1,)), ((), ())), preferred_element_type=jnp.float32
            )
            expd = jnp.exp2(scores * (float(HD) ** (-0.5) * LOG2E))
            total = jnp.sum(expd, axis=-1, keepdims=True)
            weighted = jnp.dot(
                expd.astype(jnp.bfloat16), values, preferred_element_type=jnp.float32
            ) * (1.0 / total)
            first, second = heads_at(value_off)
            return jnp.where(first, weighted[:part], jnp.where(second, weighted[part:], 0.0))

        def send_back(src, dst, send, recv):
            for k in range(part // rows - 1):
                i = k + (k >= mine).astype(jnp.int32)
                pltpu.make_async_remote_copy(
                    src_ref=src.at[pl.ds(pl.multiple_of(i * rows, rows), rows)],
                    dst_ref=dst.at[side],
                    send_sem=send,
                    recv_sem=recv.at[side],
                    device_id={"blk": half * (blks // 2) + i // 2, "uly": i % 2},
                    device_id_type=MESH,
                ).start()

            dst[side] = src[q_rows, :]

        take(qbuf.at[pl.ds(0, part - rows)], recv_q)
        stack(0, qbuf[:, 0:2 * LANES], 0)
        stack(1, qbuf[:, LANES:wide], pair - LANES)
        stack(2, qbuf[:, wide:], 0)
        gathered(0, vbuf)
        gathered(1, kbuf)
        low = attend(0, kbuf[:, 0:2 * LANES], vbuf[:, 0:2 * LANES], 0)
        high = attend(
            1, kbuf[:, LANES:wide], vbuf[:, LANES:wide], pair - LANES
        )
        four[...] = jnp.concatenate(
            [low[:, :LANES], low[:, LANES:] + high[:, :LANES], high[:, LANES:]], axis=1
        ).astype(jnp.bfloat16)
        send_back(four, back4, send4, recv4)
        gathered(2, tbuf)
        two[...] = attend(
            2, tbuf[:, 0:2 * LANES], tbuf[:, LANES:], pair - LANES
        ).astype(jnp.bfloat16)
        send_back(two, back2, send2, recv2)

    load_w.wait()
    give_w.wait_recv()

    def project(back, recv, s, start, own):
        if own:
            pl.when(jnp.logical_not(is_owner))(lambda: take(back.at[0], recv.at[s]))
        else:
            take(back.at[0], recv.at[s])
        return jnp.dot(
            back[s],
            w_vmem[pl.ds(pl.multiple_of(start, LANES // 2), back.shape[2]), :],
            preferred_element_type=jnp.float32,
        )

    def project4(s, own):
        return project(back4, recv4, s, s * last, own)

    def project2(s, own):
        return project(back2, recv2, s, wide + LANES - pair + s * pair, own)

    acc[...] = project4(side, True)
    acc[...] += project4(1 - side, False)
    acc[...] += project2(side, True)

    give_w.wait_send()
    slab = tbuf.at[pl.ds(0, rows)]
    for i in range(9):
        take(slab, send_kv)
    take(qbuf.at[pl.ds(0, rows)], send_q)
    pl.when(is_owner)(lambda: take(four.at[pl.ds(0, part - rows)], send4))

    @pl.when(jnp.logical_not(is_owner))
    def _():
        for i in range(3):
            take(slab, send_kv)
        take(qbuf.at[pl.ds(0, rows)], send_q)

    out_ref[...] = (acc[...] + project2(1 - side, False)).astype(out_ref.dtype)
    pl.when(is_owner)(lambda: take(two.at[pl.ds(0, part - rows)], send2))


def on_device_gather(blks, query, key, value, q_gain, k_gain, out_weight):
    rows, width = query.shape
    heads = width // HD
    depth, cols = out_weight.shape
    levels = blks // 2
    seq = 2 * blks * rows
    wide, pair, two = 4 * HD, 2 * HD, 2 * LANES
    dma = pltpu.SemaphoreType.DMA
    bf16 = jnp.bfloat16
    return pl.pallas_call(
        functools.partial(gather_kernel, blks, heads),
        out_shape=pltpu.VMEM((rows, cols), bf16),
        in_specs=[pl.BlockSpec(memory_space=pltpu.HBM)] * 6,
        out_specs=pl.BlockSpec(memory_space=pltpu.VMEM),
        scratch_shapes=[
            pltpu.VMEM((3, rows, width), bf16),
            pltpu.VMEM((2, 1, HD), jnp.float32),
            pltpu.VMEM((2, rows, wide), bf16),
            pltpu.VMEM((2, rows, 2 * pair), bf16),
            pltpu.VMEM((2, rows, wide + two), bf16),
            pltpu.VMEM((seq, wide), bf16),
            pltpu.VMEM((seq, wide), bf16),
            pltpu.VMEM((seq, 2 * pair), bf16),
            pltpu.VMEM((seq // 2, wide + two), bf16),
            pltpu.VMEM((seq // 2, wide), bf16),
            pltpu.VMEM((seq // 2, two), bf16),
            pltpu.VMEM((2, rows, wide), bf16),
            pltpu.VMEM((2, rows, two), bf16),
            pltpu.VMEM((rows, cols), jnp.float32),
            pltpu.VMEM((width, cols), bf16),
            pltpu.VMEM((3, seq, two), bf16),
            dma((3,)),
            dma, dma, dma, dma, dma, dma, dma,
            dma((3,)),
            dma,
            dma((2,)),
            dma((2,)),
            dma,
            pltpu.SemaphoreType.REGULAR((2,)),
        ],
        compiler_params=pltpu.CompilerParams(collective_id=0, has_side_effects=True),
    )(query, key, value, q_gain.reshape(1, HD), k_gain.reshape(1, HD), out_weight)


def fits_gather(blks, ulys, width):
    heads = width // HD
    return ulys == 2 and blks % 4 == 0 and blks <= heads and heads // 2 == 6 and width % LANES == 0


def solution(mesh):
    blks, ulys = mesh.shape["blk"], mesh.shape["uly"]
    tokens = P(("grp", "blk", "uly"), None)

    def body(query, *rest):
        if fits_gather(blks, ulys, query.shape[1]):
            return on_device_gather(blks, query, *rest)
        return on_device(blks, ulys, query, *rest)

    return jax.shard_map(
        body,
        mesh=mesh,
        in_specs=(tokens, tokens, tokens, P(), P(), P("uly", None)),
        out_specs=tokens,
        check_vma=False,
    )
```
